16 devices in a mesh: fsdp: 16 (over z, y, x, core).
Axes of the slice: x: 2, y: 2, z: 2, core: 2. Of those that a mesh axis runs over, the one named last changes fastest.
Arguments:
- tok_ids: int32 [16, 512], P('fsdp')
- tok_labels: int32 [16, 512], P('fsdp')
- embed: bfloat16 [50304, 768], P('fsdp')
- w_gate: bfloat16 [768, 3072], P('fsdp')
- w_up: bfloat16 [768, 3072], P('fsdp')
- w_down: bfloat16 [3072, 768], P('fsdp')
- gain_mlp: float32 [768], replicated
- gain_final: float32 [768], replicated
Outputs:
- output 1: float32 [], replicated
- output 2: float32 [50304, 768], P('fsdp')
- output 3: float32 [768, 3072], P('fsdp')
- output 4: float32 [768, 3072], P('fsdp')
- output 5: float32 [3072, 768], P('fsdp')
All inputs are finite; a program needn't handle non-finite values.
Results may differ from the reference program's by a relative error of at most 0.00797805.
Values are sent between devices in bfloat16 or wider.
A program may use at most 1 GiB of HBM per device.

```python
import math
import jax
import jax.numpy as jnp
from jax import lax

VOCAB_SIZE = 50304
MODEL_DIM = 768
FFN_DIM = 3072
GLOBAL_BATCH = 16
SEQ_LEN = 512
NUM_CHUNKS = 16
TOKEN_GROUPS = 16
NORM_EPS = 1e-6
CHUNK_ROWS = VOCAB_SIZE // NUM_CHUNKS
NUM_TOKENS = GLOBAL_BATCH * SEQ_LEN
GROUP_TOKENS = NUM_TOKENS // TOKEN_GROUPS
INV_TOKENS = 1.0 / NUM_TOKENS
EMB_SCALE = math.sqrt(MODEL_DIM)


def setup_inputs(seed: int = 0) -> dict:
    base_key = jax.random.key(seed)
    sub_keys = jax.random.split(base_key, 8)
    tok_ids = jax.random.randint(sub_keys[0], (GLOBAL_BATCH, SEQ_LEN), 0, VOCAB_SIZE, dtype=jnp.int32)
    tok_ids = tok_ids.at[0, 0].set(0).at[GLOBAL_BATCH - 1, SEQ_LEN - 1].set(VOCAB_SIZE - 1)
    tok_labels = jax.random.randint(sub_keys[1], (GLOBAL_BATCH, SEQ_LEN), 0, VOCAB_SIZE, dtype=jnp.int32)
    tok_labels = tok_labels.at[0, 0].set(VOCAB_SIZE - 1).at[GLOBAL_BATCH - 1, SEQ_LEN - 1].set(0)
    embed = (jax.random.normal(sub_keys[2], (VOCAB_SIZE, MODEL_DIM), jnp.float32) * MODEL_DIM ** -0.5).astype(jnp.bfloat16)
    w_gate = (jax.random.normal(sub_keys[3], (MODEL_DIM, FFN_DIM), jnp.float32) * MODEL_DIM ** -0.5).astype(jnp.bfloat16)
    w_up = (jax.random.normal(sub_keys[4], (MODEL_DIM, FFN_DIM), jnp.float32) * MODEL_DIM ** -0.5).astype(jnp.bfloat16)
    w_down = (jax.random.normal(sub_keys[5], (FFN_DIM, MODEL_DIM), jnp.float32) * (2.0 * FFN_DIM ** -0.5)).astype(jnp.bfloat16)
    gain_mlp = jax.random.uniform(sub_keys[6], (MODEL_DIM,), jnp.float32, 0.5, 1.5)
    gain_final = jax.random.uniform(sub_keys[7], (MODEL_DIM,), jnp.float32, 1.0, 2.5)
    return dict(tok_ids=tok_ids, tok_labels=tok_labels, embed=embed, w_gate=w_gate, w_up=w_up, w_down=w_down, gain_mlp=gain_mlp, gain_final=gain_final)


def rms_apply(values, gain_vec):
    inv_rms = lax.rsqrt(jnp.mean(values * values, axis=-1, keepdims=True) + NORM_EPS)
    return (values * inv_rms * gain_vec).astype(jnp.bfloat16), inv_rms


def rms_backward(values, inv_rms, gain_vec, grad_out):
    scaled = grad_out * gain_vec
    return inv_rms * scaled - values * (inv_rms ** 3) * jnp.mean(scaled * values, axis=-1, keepdims=True)


def group_grads(ids_grp, lab_grp, d_emb_acc, embed, w_gate, w_up, w_down, gain_mlp, gain_final):
    x_emb = embed[ids_grp].astype(jnp.float32) * EMB_SCALE
    normed, inv_first = rms_apply(x_emb, gain_mlp)
    gate = jnp.dot(normed, w_gate, preferred_element_type=jnp.float32).astype(jnp.bfloat16)
    up_val = jnp.dot(normed, w_up, preferred_element_type=jnp.float32).astype(jnp.bfloat16)
    gate32 = gate.astype(jnp.float32)
    up32 = up_val.astype(jnp.float32)
    hidden_act = (jax.nn.silu(gate32) * up32).astype(jnp.bfloat16)
    mlp_out = jnp.dot(hidden_act, w_down, preferred_element_type=jnp.float32).astype(jnp.bfloat16)
    hid32 = (x_emb + mlp_out.astype(jnp.float32)).astype(jnp.bfloat16).astype(jnp.float32)
    hid_norm, inv_final = rms_apply(hid32, gain_final)
    emb_chunks = embed.reshape(NUM_CHUNKS, CHUNK_ROWS, MODEL_DIM)
    chunk_index = jnp.arange(NUM_CHUNKS, dtype=jnp.int32)
    col_ids = jnp.arange(CHUNK_ROWS, dtype=jnp.int32)

    def chunk_logits(chunk_emb, chunk_idx):
        logits = jnp.dot(hid_norm, chunk_emb.T, preferred_element_type=jnp.float32)
        label_hit = (lab_grp - chunk_idx * CHUNK_ROWS)[:, None] == col_ids[None, :]
        return logits, label_hit

    def fwd_step(carry, chunk_in):
        run_max, run_sum, lab_logit = carry
        logits, label_hit = chunk_logits(chunk_in[0], chunk_in[1])
        new_max = jnp.maximum(run_max, jnp.max(logits, axis=1))
        run_sum = run_sum * jnp.exp(run_max - new_max) + jnp.sum(jnp.exp(logits - new_max[:, None]), axis=1)
        lab_logit = lab_logit + jnp.sum(jnp.where(label_hit, logits, 0.0), axis=1)
        return (new_max, run_sum, lab_logit), None

    zero_tok = jnp.zeros((GROUP_TOKENS,), jnp.float32)
    start_fwd = (jnp.full((GROUP_TOKENS,), -jnp.inf, jnp.float32), zero_tok, zero_tok)
    (run_max, run_sum, lab_logit), unused_fwd = lax.scan(fwd_step, start_fwd, (emb_chunks, chunk_index))
    log_norm = run_max + jnp.log(run_sum)
    loss_part = jnp.sum(log_norm - lab_logit)

    def bwd_step(carry, chunk_in):
        d_hid, d_rows = carry
        logits, label_hit = chunk_logits(chunk_in[0], chunk_in[1])
        prob_mat = jnp.exp(logits - log_norm[:, None])
        grad_logits = ((prob_mat - label_hit.astype(jnp.float32)) * INV_TOKENS).astype(jnp.bfloat16)
        d_rows = d_rows.at[chunk_in[1]].add(jnp.dot(grad_logits.T, hid_norm, preferred_element_type=jnp.float32))
        d_hid = d_hid + jnp.dot(grad_logits, chunk_in[0], preferred_element_type=jnp.float32)
        return (d_hid, d_rows), None

    start_bwd = (jnp.zeros((GROUP_TOKENS, MODEL_DIM), jnp.float32), d_emb_acc.reshape(NUM_CHUNKS, CHUNK_ROWS, MODEL_DIM))
    (d_hid, d_rows), unused_bwd = lax.scan(bwd_step, start_bwd, (emb_chunks, chunk_index))
    d_hidden = rms_backward(hid32, inv_final, gain_final, d_hid)
    d_mlp = d_hidden.astype(jnp.bfloat16)
    d_down = jnp.dot(hidden_act.T, d_mlp, preferred_element_type=jnp.float32)
    d_act = jnp.dot(d_mlp, w_down.T, preferred_element_type=jnp.float32)
    gate_sig = jax.nn.sigmoid(gate32)
    d_gate_pre = (d_act * up32 * gate_sig * (1.0 + gate32 * (1.0 - gate_sig))).astype(jnp.bfloat16)
    d_up_pre = (d_act * gate32 * gate_sig).astype(jnp.bfloat16)
    d_gate = jnp.dot(normed.T, d_gate_pre, preferred_element_type=jnp.float32)
    d_up = jnp.dot(normed.T, d_up_pre, preferred_element_type=jnp.float32)
    d_normed = jnp.dot(d_gate_pre, w_gate.T, preferred_element_type=jnp.float32) + jnp.dot(d_up_pre, w_up.T, preferred_element_type=jnp.float32)
    d_x = (d_hidden + rms_backward(x_emb, inv_first, gain_mlp, d_normed)).astype(jnp.bfloat16)
    d_emb_new = d_rows.reshape(VOCAB_SIZE, MODEL_DIM).at[ids_grp].add(d_x.astype(jnp.float32) * EMB_SCALE)
    return loss_part, d_emb_new, d_gate, d_up, d_down


def reference(tok_ids, tok_labels, embed, w_gate, w_up, w_down, gain_mlp, gain_final):
    ids_groups = tok_ids.reshape(TOKEN_GROUPS, GROUP_TOKENS)
    lab_groups = tok_labels.reshape(TOKEN_GROUPS, GROUP_TOKENS)

    def group_step(carry, group_in):
        loss_acc, d_emb_acc, gate_acc, up_acc, down_acc = carry
        loss_part, d_emb_acc, d_gate, d_up, d_down = group_grads(group_in[0], group_in[1], d_emb_acc, embed, w_gate, w_up, w_down, gain_mlp, gain_final)
        return (loss_acc + loss_part, d_emb_acc, gate_acc + d_gate, up_acc + d_up, down_acc + d_down), None

    start = (jnp.zeros((), jnp.float32), jnp.zeros((VOCAB_SIZE, MODEL_DIM), jnp.float32), jnp.zeros((MODEL_DIM, FFN_DIM), jnp.float32), jnp.zeros((MODEL_DIM, FFN_DIM), jnp.float32), jnp.zeros((FFN_DIM, MODEL_DIM), jnp.float32))
    totals, unused = lax.scan(group_step, start, (ids_groups, lab_groups))
    return (totals[0] * INV_TOKENS, totals[1], totals[2], totals[3], totals[4])
```

```python
import math
import jax
import jax.numpy as jnp
from jax import lax
from jax.experimental import pallas as pl
from jax.experimental.pallas import tpu as pltpu
from jax.sharding import PartitionSpec as P

NORM_EPS = 1e-6
LOG2E = 1.4426950408889634
MESH = pl.DeviceIdType.MESH
ANY = pl.BlockSpec(memory_space=pl.ANY)
VMEM = pl.BlockSpec(memory_space=pltpu.VMEM)
BF = jnp.bfloat16
F32 = jnp.float32

SHARD = 3144
HALF = 3200
VP = 2 * HALF
D = 768
FF = 3072
TOK = 512
UNIT = 256
NB = 8
TB = 512
GT = NB * TOK
VT = 1280
NT = VP // VT
NQ = NB * NT
CAP = 128
TOTAL = 8192

BLOCKS = [[(0, 0), (0, 1)], [(2, 1), (1, 1)], [(4, 1), (1, 0)], [(4, 0), (2, 0)],
          [(3, 1), (6, 1)], [(5, 1), (3, 0)], [(6, 0), (5, 0)], [(7, 0), (7, 1)]]
UNITS = [u for b in BLOCKS for u in b]
POS = {u: i for i, u in enumerate(UNITS)}


def dot_plain(a, b):
    return lax.dot_general(a, b, (((1,), (0,)), ((), ())), preferred_element_type=F32)


def dot_last(a, b):
    return lax.dot_general(a, b, (((1,), (1,)), ((), ())), preferred_element_type=F32)


def dot_first(a, b):
    return lax.dot_general(a, b, (((0,), (0,)), ((), ())), preferred_element_type=F32)


def peer_of(me, r):
    p = me
    if r & 1:
        p = p + 2 - 4 * ((me // 2) % 2)
    if r & 2:
        p = p + 4 - 8 * ((me // 4) % 2)
    if r & 4:
        p = p + 8 - 16 * (me // 8)
    return p


def barrier_with(peers):
    sem = pltpu.get_barrier_semaphore()
    for p in peers:
        pl.semaphore_signal(sem, inc=1, device_id=(p,), device_id_type=MESH)
    pl.semaphore_wait(sem, len(peers))


def remote(src, dst, ssem, rsem, dev):
    return pltpu.make_async_remote_copy(src_ref=src, dst_ref=dst, send_sem=ssem, recv_sem=rsem,
                                        device_id=(dev,), device_id_type=MESH)


def params(cid, mib=60):
    return pltpu.CompilerParams(collective_id=cid, has_side_effects=True, vmem_limit_bytes=mib * 2 ** 20)


def pair_kernel(e_ref, out_ref, buf, zero, sems, ssem, rsem):
    me = lax.axis_index('fsdp')
    other = me + 1 - 2 * (me % 2)
    barrier_with([other])
    load = pltpu.make_async_copy(e_ref, buf, sems.at[0])
    load.start()
    zero[...] = jnp.zeros_like(zero)
    load.wait()
    send = remote(buf, out_ref.at[pl.ds(HALF, SHARD)], ssem, rsem, other)
    send.start()
    copies = [pltpu.make_async_copy(buf, out_ref.at[pl.ds(0, SHARD)], sems.at[1]),
              pltpu.make_async_copy(zero, out_ref.at[pl.ds(SHARD, HALF - SHARD)], sems.at[2]),
              pltpu.make_async_copy(zero, out_ref.at[pl.ds(HALF + SHARD, HALF - SHARD)], sems.at[3])]
    for c in copies:
        c.start()
    for c in copies:
        c.wait()
    send.wait()


def pair_gather(e_shard):
    return pl.pallas_call(
        pair_kernel, in_specs=[ANY], out_specs=ANY, out_shape=jax.ShapeDtypeStruct((VP, D), BF),
        scratch_shapes=[pltpu.VMEM((SHARD, D), BF), pltpu.VMEM((HALF - SHARD, D), BF), pltpu.SemaphoreType.DMA((4,)),
                        pltpu.SemaphoreType.DMA, pltpu.SemaphoreType.DMA],
        compiler_params=params(0, 16), name='pair_gather')(e_shard)


def swap_kernel(in_ref, out_ref, recv, ssem, rsem):
    me = lax.axis_index('fsdp')
    peers = [peer_of(me, r) for r in range(1, NB)]
    barrier_with(peers)
    sends = [remote(in_ref.at[r], recv.at[r], ssem.at[r], rsem.at[r], peers[r - 1]) for r in range(1, NB)]
    for s in sends:
        s.start()
    out_ref[0] = in_ref[0]
    for r in range(1, NB):
        sends[r - 1].wait()
        out_ref[r] = recv[r]


def swap(rows, cid):
    return pl.pallas_call(
        swap_kernel, in_specs=[VMEM], out_specs=VMEM, out_shape=jax.ShapeDtypeStruct((NB, CAP, D), BF),
        scratch_shapes=[pltpu.VMEM((NB, CAP, D), BF), pltpu.SemaphoreType.DMA((NB,)), pltpu.SemaphoreType.DMA((NB,))],
        compiler_params=params(cid, 16), name='swap')(rows)


def mask_pads(s, j):
    @pl.when(j == 2)
    def _():
        s[pl.ds(SHARD - 2 * VT, HALF - SHARD), :] = jnp.full((HALF - SHARD, TB), -jnp.inf, F32)

    @pl.when(j == 4)
    def _():
        s[pl.ds(HALF + SHARD - 4 * VT, HALF - SHARD), :] = jnp.full((HALF - SHARD, TB), -jnp.inf, F32)


AG_PATHS = ([(0, a, 0, D) for a in range(3)] + [(2, 0, 0, D), (4, 1, 0, D), (1, 2, 0, D)]
            + [(6, 0, 0, 256), (5, 1, 256, 512), (3, 2, 512, D)])
AG_LIST = [(s, h, a, lo, hi) for h in (1, 0) for (s, a, lo, hi) in AG_PATHS]


def fwd_kernel(hn_ref, e_ref, all_ref, lse_ref, e_v, hn_s, s0, s1, st, stat, csem, ssem, rsem, ssem2, rsem2):
    me = lax.axis_index('fsdp')
    nbr = [peer_of(me, 1 << a) for a in range(3)]
    peers = [peer_of(me, r) for r in range(1, NB)]
    barrier_with(peers)
    load_e = pltpu.make_async_copy(e_ref, e_v, csem.at[0])
    load_e.start()
    load_h = pltpu.make_async_copy(hn_ref, hn_s.at[pl.ds(0, TOK)], csem.at[1])
    load_h.start()
    load_h.wait()

    def piece(k):
        s, h, a, lo, hi = AG_LIST[k]
        src = hn_s.at[pl.ds(POS[(s, h)] * UNIT, UNIT), pl.ds(lo, hi - lo)]
        dst = hn_s.at[pl.ds(POS[(s ^ (1 << a), h)] * UNIT, UNIT), pl.ds(lo, hi - lo)]
        return remote(src, dst, ssem.at[k], rsem.at[k], nbr[a])

    def forward(unit):
        for k, (s, h, a, lo, hi) in enumerate(AG_LIST):
            if (s, h) == unit:
                piece(k).start()

    def arrive(units):
        for unit in units:
            for k, (s, h, a, lo, hi) in enumerate(AG_LIST):
                if (s ^ (1 << a), h) == unit:
                    piece(k).wait_recv()
            forward(unit)

    forward((0, 1))
    forward((0, 0))
    st[:, 0] = jnp.full((NB, 8, TB), -jnp.inf, F32)
    st[:, 1] = jnp.zeros((NB, 8, TB), F32)
    load_e.wait()

    def sdot(q):
        off = pl.multiple_of(lax.rem(q, NT) * VT, VT)
        tok = pl.multiple_of(lax.div(q, NT) * TB, TB)
        return dot_last(e_v[pl.ds(off, VT), :], hn_s[pl.ds(tok, TB), :])

    def proc(q, s):
        mask_pads(s, lax.rem(q, NT))
        blk = lax.div(q, NT)
        s3 = s[...].reshape(VT // 8, 8, TB)
        m8 = st[blk, 0]
        nm = jnp.maximum(m8, s3.max(0))
        st[blk, 1] = st[blk, 1] * jnp.exp2((m8 - nm) * LOG2E) + jnp.exp2((s3 - nm[None]) * LOG2E).sum(0)
        st[blk, 0] = nm

    s0[...] = sdot(0)

    def body(i, carry):
        q = 2 * i
        for block, units in ((1, [(2, 1), (1, 1), (4, 1)]), (2, [(1, 0), (4, 0), (2, 0)]),
                             (4, [(3, 1), (6, 1), (5, 1)]), (5, [(3, 0), (6, 0), (5, 0)]), (7, [(7, 0), (7, 1)])):
            @pl.when(i == (block * NT - 1) // 2)
            def _(units=units):
                arrive(units)
        s1[...] = sdot(q + 1)
        proc(q, s0)
        s0[...] = sdot(jnp.minimum(q + 2, NQ - 1))
        proc(q + 1, s1)
        return carry

    lax.fori_loop(0, NQ // 2, body, 0)
    out = pltpu.make_async_copy(hn_s, all_ref, csem.at[2])
    out.start()

    def unit_stat(unit):
        blk, at = POS[unit] // 2, (POS[unit] % 2) * UNIT
        m8, s8 = st[blk, 0, :, at:at + UNIT], st[blk, 1, :, at:at + UNIT]
        m = m8.max(0, keepdims=True)
        return m, (s8 * jnp.exp2((m8 - m) * LOG2E)).sum(0, keepdims=True)

    for r in range(NB):
        for h in range(2):
            m, s = unit_stat((r, h))
            stat[0, 2 * r:2 * r + 1, h * UNIT:(h + 1) * UNIT] = m
            stat[0, 2 * r + 1:2 * r + 2, h * UNIT:(h + 1) * UNIT] = s
    sends = [remote(stat.at[0], stat.at[r], ssem2.at[r], rsem2.at[r], peers[r - 1]) for r in range(1, NB)]
    for c in sends:
        c.start()
    for c in sends:
        c.wait()
    for r in range(NB):
        ms = [stat[k, 2 * (k ^ r):2 * (k ^ r) + 1, :] for k in range(NB)]
        ss = [stat[k, 2 * (k ^ r) + 1:2 * (k ^ r) + 2, :] for k in range(NB)]
        top = ms[0]
        for m in ms[1:]:
            top = jnp.maximum(top, m)
        tot = jnp.zeros_like(top)
        for m, s in zip(ms, ss):
            tot = tot + s * jnp.exp2((m - top) * LOG2E)
        lse = top + jnp.log(tot)
        for h in range(2):
            blk, at = POS[(r, h)] // 2, (POS[(r, h)] % 2) * UNIT
            lse_ref[blk, :, at:at + UNIT] = lse[:, h * UNIT:(h + 1) * UNIT]
    for k in range(len(AG_LIST)):
        piece(k).wait_send()
    out.wait()


def head_forward(hn, e_loc):
    n = len(AG_LIST)
    return pl.pallas_call(
        fwd_kernel, in_specs=[ANY, ANY], out_specs=[ANY, VMEM],
        out_shape=[jax.ShapeDtypeStruct((GT, D), BF), jax.ShapeDtypeStruct((NB, 1, TB), F32)],
        scratch_shapes=[pltpu.VMEM((VP, D), BF), pltpu.VMEM((GT, D), BF), pltpu.VMEM((VT, TB), F32), pltpu.VMEM((VT, TB), F32),
                        pltpu.VMEM((NB, 2, 8, TB), F32), pltpu.VMEM((NB, 16, TB), F32), pltpu.SemaphoreType.DMA((3,)),
                        pltpu.SemaphoreType.DMA((n,)), pltpu.SemaphoreType.DMA((n,)),
                        pltpu.SemaphoreType.DMA((NB,)), pltpu.SemaphoreType.DMA((NB,))],
        compiler_params=params(1), name='head_fwd')(hn, e_loc)


RS_PATHS = [(7, 0, 0, 256), (7, 1, 256, 512), (7, 2, 512, D),
            (5, 2, 0, 384), (5, 0, 384, D), (6, 1, 0, 384), (6, 2, 384, D), (3, 0, 0, 384), (3, 1, 384, D),
            (1, 0, 0, D), (2, 1, 0, D), (4, 2, 0, D)]
RS_LIST = [(s, h, a, lo, hi) for (s, a, lo, hi) in RS_PATHS for h in range(2)]


def rs_place(k):
    s, h, a, lo, hi = RS_LIST[k]
    t = s ^ (1 << a)
    if s == 7:
        return 0, {6: 0, 5: 1, 3: 2}[t] * 2 + h, 0
    if t:
        return 1, {1: 0, 2: 1, 4: 2}[t] * 2 + h, lo
    return 2, a * 2 + h, 0


def bwd_kernel(hn_ref, e_ref, lse_ref, lab_ref, dh_ref, g_ref, l_ref,
               e_v, hn_s, s0, s1, g0, g1, dh, ra, rb, rc, csem, gsem, ssem, rsem):
    me = lax.axis_index('fsdp')
    nbr = [peer_of(me, 1 << a) for a in range(3)]
    barrier_with(nbr)
    load_e = pltpu.make_async_copy(e_ref, e_v, csem.at[0])
    load_e.start()
    load_h = pltpu.make_async_copy(hn_ref, hn_s, csem.at[1])
    load_h.start()
    dh[...] = jnp.zeros_like(dh)
    l_ref[...] = jnp.zeros_like(l_ref)
    bufs = (ra, rb, rc)

    def piece(k):
        s, h, a, lo, hi = RS_LIST[k]
        src = dh.at[pl.ds(POS[(s, h)] * UNIT, UNIT), pl.ds(lo, hi - lo)]
        b, i, c = rs_place(k)
        return remote(src, bufs[b].at[i, :, pl.ds(c, hi - lo)], ssem.at[k], rsem.at[k], nbr[a])

    def finish(block):
        for unit in BLOCKS[block]:
            rows = pl.ds(POS[unit] * UNIT, UNIT)
            for k, (s, h, a, lo, hi) in enumerate(RS_LIST):
                if (s ^ (1 << a), h) == unit:
                    piece(k).wait_recv()
                    b, i, c = rs_place(k)
                    dh[rows, lo:hi] += bufs[b][i, :, c:c + hi - lo]
            for k, (s, h, a, lo, hi) in enumerate(RS_LIST):
                if (s, h) == unit:
                    piece(k).start()

    def place(q):
        return NB - 1 - lax.div(q, NT), pl.multiple_of(lax.rem(q, NT) * VT, VT)

    def sdot(q):
        blk, off = place(q)
        return dot_last(e_v[pl.ds(off, VT), :], hn_s[pl.ds(pl.multiple_of(blk * TB, TB), TB), :])

    iota = lax.broadcasted_iota(jnp.int32, (VT, TB), 0)

    def g_copy(q, g, k):
        blk, off = place(q)
        return pltpu.make_async_copy(g, g_ref.at[pl.ds(off, VT), pl.ds(pl.multiple_of(blk * TB, TB), TB)], gsem.at[k])

    def proc(q, s, g, k):
        blk, off = place(q)
        mask_pads(s, lax.rem(q, NT))

        @pl.when(q >= 2)
        def _():
            g_copy(q, g, k).wait()
        w = s[...] - lse_ref[blk]
        hit = iota == (lab_ref[blk] - off)
        p = jnp.exp2(w * LOG2E - 13.0)
        gv = (p - jnp.where(hit, 2.0 ** -13, 0.0)).astype(BF)
        l_ref[...] += jnp.where(hit, w, 0.0).reshape(VT // 8, 8, TB).sum(0)
        g[...] = gv
        rows = pl.ds(pl.multiple_of(blk * TB, TB), TB)
        dh[rows, :] += dot_first(gv, e_v[pl.ds(off, VT), :])

    def after(q, g, k):
        g_copy(q, g, k).start()
        for i in range(NB):
            @pl.when(q == i * NT + NT - 1)
            def _(i=i):
                finish(NB - 1 - i)

    load_e.wait()
    load_h.wait()
    s0[...] = sdot(0)

    def body(i, carry):
        q = 2 * i
        s1[...] = sdot(q + 1)
        proc(q, s0, g0, 0)
        after(q, g0, 0)
        s0[...] = sdot(jnp.minimum(q + 2, NQ - 1))
        proc(q + 1, s1, g1, 1)
        after(q + 1, g1, 1)
        return carry

    lax.fori_loop(0, NQ // 2, body, 0)
    g_copy(NQ - 2, g0, 0).wait()
    g_copy(NQ - 1, g1, 1).wait()
    dh_ref[...] = dh[pl.ds(0, TOK), :]
    for k in range(len(RS_LIST)):
        piece(k).wait_send()


def head_backward(hn_all, e_loc, lse, lab):
    n = len(RS_LIST)
    return pl.pallas_call(
        bwd_kernel, in_specs=[ANY, ANY, VMEM, VMEM], out_specs=[VMEM, ANY, VMEM],
        out_shape=[jax.ShapeDtypeStruct((TOK, D), F32), jax.ShapeDtypeStruct((VP, GT), BF), jax.ShapeDtypeStruct((8, TB), F32)],
        scratch_shapes=[pltpu.VMEM((VP, D), BF), pltpu.VMEM((GT, D), BF), pltpu.VMEM((VT, TB), F32), pltpu.VMEM((VT, TB), F32),
                        pltpu.VMEM((VT, TB), BF), pltpu.VMEM((VT, TB), BF), pltpu.VMEM((GT, D), F32),
                        pltpu.VMEM((6, UNIT, 256), F32), pltpu.VMEM((6, UNIT, D), F32), pltpu.VMEM((6, UNIT, D), F32),
                        pltpu.SemaphoreType.DMA((2,)), pltpu.SemaphoreType.DMA((2,)),
                        pltpu.SemaphoreType.DMA((n,)), pltpu.SemaphoreType.DMA((n,))],
        compiler_params=params(2), name='head_bwd')(hn_all, e_loc, lse, lab)


DE_T = 640


def de_kernel(scale, g_ref, hn_ref, rows_ref, dx_ref, out_ref):
    out_ref[...] = dot_plain(g_ref[...], hn_ref[...])
    base = pl.program_id(0) * DE_T
    iota = lax.broadcasted_iota(jnp.int32, (DE_T, NB * CAP), 0)
    pick = jnp.where(iota == rows_ref[...] - base, 1.0, 0.0).astype(BF)
    out_ref[...] += dot_plain(pick, dx_ref[...]) * scale


def embed_grad(g, hn_all, rows, dx, scale):
    import functools
    n = NB * CAP
    return pl.pallas_call(
        functools.partial(de_kernel, scale), grid=(VP // DE_T,),
        in_specs=[pl.BlockSpec((DE_T, GT), lambda j: (j, 0)), pl.BlockSpec((GT, D), lambda j: (0, 0)),
                  pl.BlockSpec((1, n), lambda j: (0, 0)), pl.BlockSpec((n, D), lambda j: (0, 0))],
        out_specs=pl.BlockSpec((DE_T, D), lambda j: (j, 0)), out_shape=jax.ShapeDtypeStruct((VP, D), F32),
        compiler_params=pltpu.CompilerParams(vmem_limit_bytes=60 * 2 ** 20),
        cost_estimate=pl.CostEstimate(flops=2 * VP * (GT + n) * D, bytes_accessed=VP * GT * 2 + VP * D * 4, transcendentals=0),
        name='embed_grad')(g, hn_all, rows, dx)


def rms_apply(values, gain_vec):
    inv_rms = lax.rsqrt(jnp.mean(values * values, axis=-1, keepdims=True) + NORM_EPS)
    return (values * inv_rms * gain_vec).astype(BF), inv_rms


def rms_backward(values, inv_rms, gain_vec, grad_out):
    scaled = grad_out * gain_vec
    return inv_rms * scaled - values * (inv_rms ** 3) * jnp.mean(scaled * values, axis=-1, keepdims=True)


def solution(mesh):
    def local_step(ids_blk, lab_blk, emb_shard, gate_shard, up_shard, down_shard, gain_mlp, gain_final):
        me = lax.axis_index('fsdp')
        core, chip = me % 2, me // 2
        scale = math.sqrt(D)
        both = lax.all_gather(jnp.concatenate([ids_blk, lab_blk]), 'fsdp')
        w_gu = lax.all_gather(jnp.concatenate([gate_shard, up_shard], 1), 'fsdp', tiled=True)
        w_down = lax.all_gather(down_shard, 'fsdp', tiled=True)
        e_loc = pair_gather(emb_shard)

        rel = jnp.stack([peer_of(me, r) for r in range(NB)])
        grp = jnp.take(both, rel, axis=0)
        ids, labs = grp[:, 0], grp[:, 1]

        def local_row(v):
            within = v % (2 * SHARD)
            row = jnp.where(within // SHARD == core, 0, HALF) + within % SHARD
            return jnp.where(v // (2 * SHARD) == chip, row, -1)

        rows = local_row(ids)
        lab_row = local_row(labs)
        mine = (rows >= 0).astype(F32)
        before = (jnp.arange(TOK)[:, None] < jnp.arange(TOK)[None, :]).astype(F32)
        rank = dot_plain(mine, before).astype(jnp.int32)
        slots = jnp.arange(CAP, dtype=jnp.int32)
        own_chip = ids[0] // (2 * SHARD)
        own_rel = jnp.bitwise_xor(own_chip, chip)
        is_rel = own_rel[None, :] == jnp.arange(NB)[:, None]
        own_rank_all = dot_plain(is_rel.astype(F32), before)
        own_rank = jnp.sum(jnp.where(is_rel, own_rank_all, 0.0), 0).astype(jnp.int32)
        counts = jnp.sum((both[:, 0] // (2 * SHARD))[:, None, :] == jnp.arange(NB)[None, :, None], axis=-1)
        rounds = (jnp.max(counts) + CAP - 1) // CAP

        def slot_rows(rnd):
            want = (rows[:, None, :] >= 0) & (rank[:, None, :] - rnd * CAP == slots[None, :, None])
            got = jnp.sum(jnp.where(want, rows[:, None, :] + 1, 0), axis=-1) - 1
            return got.reshape(NB * CAP)

        def slot_tokens(rnd):
            want = is_rel[:, None, :] & (own_rank[None, None, :] - rnd * CAP == slots[None, :, None])
            return jnp.sum(jnp.where(want, jnp.arange(TOK)[None, None, :], 0), axis=-1).reshape(NB * CAP)

        def lookup(rnd, x, cid):
            out = jnp.take(e_loc, jnp.maximum(slot_rows(rnd), 0), axis=0, mode='clip').reshape(NB, CAP, D)
            got = swap(out, cid).reshape(NB * CAP, D)
            here = own_rank // CAP == rnd
            at = jnp.where(here, own_rel * CAP + own_rank % CAP, 0)
            return jnp.where(here[:, None], jnp.take(got, at, axis=0, mode='clip'), x)

        x_bf = lookup(0, jnp.zeros((TOK, D), BF), 3)
        x_bf = lax.while_loop(lambda c: c[0] < rounds, lambda c: (c[0] + 1, lookup(c[0], c[1], 4)), (jnp.int32(1), x_bf))[1]

        x_emb = x_bf.astype(F32) * scale
        normed, inv_first = rms_apply(x_emb, gain_mlp)
        gu = dot_plain(normed, w_gu).astype(BF)
        gate, up_val = gu[:, :FF].astype(F32), gu[:, FF:].astype(F32)
        hidden_act = (jax.nn.silu(gate) * up_val).astype(BF)
        mlp_out = dot_plain(hidden_act, w_down).astype(BF)
        hid32 = (x_emb + mlp_out.astype(F32)).astype(BF).astype(F32)
        hid_norm, inv_final = rms_apply(hid32, gain_final)

        hn_all, lse = head_forward(hid_norm, e_loc)
        lab_pos = jnp.concatenate([lab_row[r, h * UNIT:(h + 1) * UNIT] for r, h in UNITS]).reshape(NB, 1, TB)
        d_hid, g_all, loss8 = head_backward(hn_all, e_loc, lse, lab_pos)
        loss = lax.psum(-jnp.sum(loss8), 'fsdp') * (1.0 / TOTAL)

        d_hidden = rms_backward(hid32, inv_final, gain_final, d_hid)
        d_mlp = d_hidden.astype(BF)
        d_down = lax.psum_scatter(dot_first(hidden_act, d_mlp), 'fsdp', scatter_dimension=0, tiled=True)
        d_act = dot_last(d_mlp, w_down)
        sig = jax.nn.sigmoid(gate)
        d_gate_pre = (d_act * up_val * sig * (1.0 + gate * (1.0 - sig))).astype(BF)
        d_up_pre = (d_act * gate * sig).astype(BF)
        d_gu_pre = jnp.concatenate([d_gate_pre, d_up_pre], 1)
        d_gu = lax.psum_scatter(dot_first(normed, d_gu_pre), 'fsdp', scatter_dimension=0, tiled=True)
        d_normed = dot_last(d_gu_pre, w_gu)
        d_x = (d_hidden + rms_backward(x_emb, inv_first, gain_mlp, d_normed)).astype(BF)

        def send_dx(rnd, cid):
            return swap(jnp.take(d_x, slot_tokens(rnd), axis=0, mode='clip').reshape(NB, CAP, D), cid).reshape(NB * CAP, D)

        d_loc = embed_grad(g_all, hn_all, slot_rows(0)[None, :], send_dx(0, 5), scale)

        def more(c):
            rnd, acc = c
            at = slot_rows(rnd)
            add = jnp.where((at >= 0)[:, None], send_dx(rnd, 6).astype(F32) * scale, 0.0)
            return rnd + 1, acc.at[jnp.maximum(at, 0)].add(add)

        d_loc = lax.while_loop(lambda c: c[0] < rounds, more, (jnp.int32(1), d_loc))[1]
        pairs = [(d, d ^ 1) for d in range(2 * NB)]
        d_embed = d_loc[:SHARD] + lax.ppermute(d_loc[HALF:HALF + SHARD], 'fsdp', pairs)
        return loss, d_embed, d_gu[:, :FF], d_gu[:, FF:], d_down

    shard = P('fsdp', None)
    return jax.shard_map(local_step, mesh=mesh, in_specs=(shard,) * 6 + (P(), P()),
                         out_specs=(P(), shard, shard, shard, shard), check_vma=False)
```

```python
import functools
import math
import jax
import jax.numpy as jnp
from jax import lax
from jax.experimental import pallas as pl
from jax.experimental.pallas import tpu as pltpu
from jax.sharding import PartitionSpec as P

NORM_EPS = 1e-6
LOG2E = 1.4426950408889634
MESH = pl.DeviceIdType.MESH
ANY = pl.BlockSpec(memory_space=pl.ANY)
VMEM = pl.BlockSpec(memory_space=pltpu.VMEM)
BF = jnp.bfloat16
F32 = jnp.float32

SHARD = 3144
HALF = 3200
VP = 2 * HALF
D = 768
FF = 3072
TOK = 512
UNIT = 256
NB = 8
TB = 512
GT = NB * TOK
VT = 1280
NT = VP // VT
NQ = NB * NT
CAP = 128
TOTAL = 8192
EMB_SCALE = math.sqrt(D)

BLOCKS = [[(0, 0), (0, 1)], [(2, 1), (1, 1)], [(4, 1), (1, 0)], [(4, 0), (2, 0)],
          [(3, 1), (6, 1)], [(5, 1), (3, 0)], [(6, 0), (5, 0)], [(7, 0), (7, 1)]]
UNITS = [u for b in BLOCKS for u in b]
POS = {u: i for i, u in enumerate(UNITS)}


def dot_plain(a, b):
    return lax.dot_general(a, b, (((1,), (0,)), ((), ())), preferred_element_type=F32)


def dot_last(a, b):
    return lax.dot_general(a, b, (((1,), (1,)), ((), ())), preferred_element_type=F32)


def dot_first(a, b):
    return lax.dot_general(a, b, (((0,), (0,)), ((), ())), preferred_element_type=F32)


def peer_of(me, r):
    p = me
    if r & 1:
        p = p + 2 - 4 * ((me // 2) % 2)
    if r & 2:
        p = p + 4 - 8 * ((me // 4) % 2)
    if r & 4:
        p = p + 8 - 16 * (me // 8)
    return p


def barrier_with(peers):
    sem = pltpu.get_barrier_semaphore()
    for p in peers:
        pl.semaphore_signal(sem, inc=1, device_id=(p,), device_id_type=MESH)
    pl.semaphore_wait(sem, len(peers))


def remote(src, dst, ssem, rsem, dev):
    return pltpu.make_async_remote_copy(src_ref=src, dst_ref=dst, send_sem=ssem, recv_sem=rsem,
                                        device_id=(dev,), device_id_type=MESH)


def params(cid, mib=60):
    return pltpu.CompilerParams(collective_id=cid, has_side_effects=True, vmem_limit_bytes=mib * 2 ** 20)


def pair_kernel(e_ref, out_ref, buf, zero, sems, ssem, rsem):
    me = lax.axis_index('fsdp')
    other = me + 1 - 2 * (me % 2)
    barrier_with([other])
    load = pltpu.make_async_copy(e_ref, buf, sems.at[0])
    load.start()
    zero[...] = jnp.zeros_like(zero)
    load.wait()
    send = remote(buf, out_ref.at[pl.ds(HALF, SHARD)], ssem, rsem, other)
    send.start()
    copies = [pltpu.make_async_copy(buf, out_ref.at[pl.ds(0, SHARD)], sems.at[1]),
              pltpu.make_async_copy(zero, out_ref.at[pl.ds(SHARD, HALF - SHARD)], sems.at[2]),
              pltpu.make_async_copy(zero, out_ref.at[pl.ds(HALF + SHARD, HALF - SHARD)], sems.at[3])]
    for c in copies:
        c.start()
    for c in copies:
        c.wait()
    send.wait()


def pair_gather(e_shard):
    return pl.pallas_call(
        pair_kernel, in_specs=[ANY], out_specs=ANY, out_shape=jax.ShapeDtypeStruct((VP, D), BF),
        scratch_shapes=[pltpu.VMEM((SHARD, D), BF), pltpu.VMEM((HALF - SHARD, D), BF), pltpu.SemaphoreType.DMA((4,)),
                        pltpu.SemaphoreType.DMA, pltpu.SemaphoreType.DMA],
        compiler_params=params(0, 16), name='pair_gather')(e_shard)


def swap_kernel(in_ref, out_ref, recv, ssem, rsem):
    me = lax.axis_index('fsdp')
    peers = [peer_of(me, r) for r in range(1, NB)]
    barrier_with(peers)
    sends = [remote(in_ref.at[r], recv.at[r], ssem.at[r], rsem.at[r], peers[r - 1]) for r in range(1, NB)]
    for s in sends:
        s.start()
    out_ref[0] = in_ref[0]
    for r in range(1, NB):
        sends[r - 1].wait()
        out_ref[r] = recv[r]


def swap(rows, cid):
    return pl.pallas_call(
        swap_kernel, in_specs=[VMEM], out_specs=VMEM, out_shape=jax.ShapeDtypeStruct((NB, CAP, D), BF),
        scratch_shapes=[pltpu.VMEM((NB, CAP, D), BF), pltpu.SemaphoreType.DMA((NB,)), pltpu.SemaphoreType.DMA((NB,))],
        compiler_params=params(cid, 16), name='swap')(rows)


def mask_pads(s, j):
    for tile, at in ((2, SHARD - 2 * VT), (4, HALF + SHARD - 4 * VT)):
        rows = pl.ds(at, HALF - SHARD)
        s[rows, :] = jnp.where(j == tile, -jnp.inf, s[rows, :])


AG_PATHS = ([(0, a, 0, D) for a in range(3)] + [(2, 0, 0, D), (4, 1, 0, D), (1, 2, 0, D)]
            + [(6, 0, 0, 256), (5, 1, 256, 512), (3, 2, 512, D)])
AG_LIST = [(s, h, a, lo, hi) for h in (1, 0) for (s, a, lo, hi) in AG_PATHS]


def fwd_kernel(hn_ref, e_ref, all_ref, lse_ref, e_v, hn_s, s0, s1, st, stat, csem, ssem, rsem, ssem2, rsem2):
    me = lax.axis_index('fsdp')
    nbr = [peer_of(me, 1 << a) for a in range(3)]
    peers = [peer_of(me, r) for r in range(1, NB)]
    barrier_with(peers)
    load_e = pltpu.make_async_copy(e_ref, e_v, csem.at[0])
    load_e.start()
    load_h = pltpu.make_async_copy(hn_ref, hn_s.at[pl.ds(0, TOK)], csem.at[1])
    load_h.start()
    load_h.wait()

    def piece(k):
        s, h, a, lo, hi = AG_LIST[k]
        src = hn_s.at[pl.ds(POS[(s, h)] * UNIT, UNIT), pl.ds(lo, hi - lo)]
        dst = hn_s.at[pl.ds(POS[(s ^ (1 << a), h)] * UNIT, UNIT), pl.ds(lo, hi - lo)]
        return remote(src, dst, ssem.at[k], rsem.at[k], nbr[a])

    def forward(unit):
        for k, (s, h, a, lo, hi) in enumerate(AG_LIST):
            if (s, h) == unit:
                piece(k).start()

    def arrive(units):
        for unit in units:
            for k, (s, h, a, lo, hi) in enumerate(AG_LIST):
                if (s ^ (1 << a), h) == unit:
                    piece(k).wait_recv()
            forward(unit)

    forward((0, 1))
    forward((0, 0))
    st[:, 0] = jnp.full((NB, 8, TB), -jnp.inf, F32)
    st[:, 1] = jnp.zeros((NB, 8, TB), F32)
    load_e.wait()

    def sdot(q):
        off = pl.multiple_of(lax.rem(q, NT) * VT, VT)
        tok = pl.multiple_of(lax.div(q, NT) * TB, TB)
        return dot_last(e_v[pl.ds(off, VT), :], hn_s[pl.ds(tok, TB), :])

    def proc(q, s):
        blk = lax.div(q, NT)
        s3 = s[...].reshape(VT // 8, 8, TB)
        m8 = st[blk, 0]
        nm = jnp.maximum(m8, s3.max(0))
        st[blk, 1] = st[blk, 1] * jnp.exp2((m8 - nm) * LOG2E) + jnp.exp2((s3 - nm[None]) * LOG2E).sum(0)
        st[blk, 0] = nm

    s0[...] = sdot(0)

    def body(i, carry):
        q = 2 * i
        for block, units in ((1, [(2, 1), (1, 1), (4, 1)]), (2, [(1, 0), (4, 0), (2, 0)]),
                             (4, [(3, 1), (6, 1), (5, 1)]), (5, [(3, 0), (6, 0), (5, 0)]), (7, [(7, 0), (7, 1)])):
            @pl.when(i == (block * NT - 1) // 2)
            def _(units=units):
                arrive(units)
        s1[...] = sdot(q + 1)
        mask_pads(s0, lax.rem(q, NT))
        proc(q, s0)
        s0[...] = sdot(jnp.minimum(q + 2, NQ - 1))
        mask_pads(s1, lax.rem(q + 1, NT))
        proc(q + 1, s1)
        return carry

    lax.fori_loop(0, NQ // 2, body, 0)
    out = pltpu.make_async_copy(hn_s, all_ref, csem.at[2])
    out.start()

    def unit_stat(unit):
        blk, at = POS[unit] // 2, (POS[unit] % 2) * UNIT
        m8, s8 = st[blk, 0, :, at:at + UNIT], st[blk, 1, :, at:at + UNIT]
        m = m8.max(0, keepdims=True)
        return m, (s8 * jnp.exp2((m8 - m) * LOG2E)).sum(0, keepdims=True)

    for r in range(NB):
        for h in range(2):
            m, s = unit_stat((r, h))
            stat[0, 2 * r:2 * r + 1, h * UNIT:(h + 1) * UNIT] = m
            stat[0, 2 * r + 1:2 * r + 2, h * UNIT:(h + 1) * UNIT] = s
    sends = [remote(stat.at[0], stat.at[r], ssem2.at[r], rsem2.at[r], peers[r - 1]) for r in range(1, NB)]
    for c in sends:
        c.start()
    for c in sends:
        c.wait()
    for r in range(NB):
        ms = [stat[k, 2 * (k ^ r):2 * (k ^ r) + 1, :] for k in range(NB)]
        ss = [stat[k, 2 * (k ^ r) + 1:2 * (k ^ r) + 2, :] for k in range(NB)]
        top = ms[0]
        for m in ms[1:]:
            top = jnp.maximum(top, m)
        tot = jnp.zeros_like(top)
        for m, s in zip(ms, ss):
            tot = tot + s * jnp.exp2((m - top) * LOG2E)
        lse = top + jnp.log(tot)
        for h in range(2):
            blk, at = POS[(r, h)] // 2, (POS[(r, h)] % 2) * UNIT
            lse_ref[blk, :, at:at + UNIT] = lse[:, h * UNIT:(h + 1) * UNIT]
    for k in range(len(AG_LIST)):
        piece(k).wait_send()
    out.wait()


def head_forward(hn, e_loc):
    n = len(AG_LIST)
    return pl.pallas_call(
        fwd_kernel, in_specs=[ANY, ANY], out_specs=[ANY, VMEM],
        out_shape=[jax.ShapeDtypeStruct((GT, D), BF), jax.ShapeDtypeStruct((NB, 1, TB), F32)],
        scratch_shapes=[pltpu.VMEM((VP, D), BF), pltpu.VMEM((GT, D), BF), pltpu.VMEM((VT, TB), F32), pltpu.VMEM((VT, TB), F32),
                        pltpu.VMEM((NB, 2, 8, TB), F32), pltpu.VMEM((NB, 16, TB), F32), pltpu.SemaphoreType.DMA((3,)),
                        pltpu.SemaphoreType.DMA((n,)), pltpu.SemaphoreType.DMA((n,)),
                        pltpu.SemaphoreType.DMA((NB,)), pltpu.SemaphoreType.DMA((NB,))],
        compiler_params=params(1), name='head_fwd')(hn, e_loc)


RS_PATHS = [(7, 0, 0, 256), (7, 1, 256, 512), (7, 2, 512, D),
            (5, 2, 0, 384), (5, 0, 384, D), (6, 1, 0, 384), (6, 2, 384, D), (3, 0, 0, 384), (3, 1, 384, D),
            (1, 0, 0, D), (2, 1, 0, D), (4, 2, 0, D)]
RS_LIST = [(s, h, a, lo, hi) for (s, a, lo, hi) in RS_PATHS for h in range(2)]


def rs_place(k):
    s, h, a, lo, hi = RS_LIST[k]
    t = s ^ (1 << a)
    if s == 7:
        return 0, {6: 0, 5: 1, 3: 2}[t] * 2 + h, 0
    if t:
        return 1, {1: 0, 2: 1, 4: 2}[t] * 2 + h, lo
    return 2, a * 2 + h, 0


def bwd_kernel(hn_ref, e_ref, lse_ref, lab_ref, dh_ref, g_ref, l_ref,
               e_v, hn_s, s0, s1, g_s, dh, ra, rb, rc, csem, gsem, ssem, rsem):
    me = lax.axis_index('fsdp')
    nbr = [peer_of(me, 1 << a) for a in range(3)]
    barrier_with(nbr)
    load_e = pltpu.make_async_copy(e_ref, e_v, csem.at[0])
    load_e.start()
    load_h = pltpu.make_async_copy(hn_ref, hn_s, csem.at[1])
    load_h.start()
    dh[...] = jnp.zeros_like(dh)
    l_ref[...] = jnp.zeros_like(l_ref)
    bufs = (ra, rb, rc)

    def piece(k):
        s, h, a, lo, hi = RS_LIST[k]
        src = dh.at[pl.ds(POS[(s, h)] * UNIT, UNIT), pl.ds(lo, hi - lo)]
        b, i, c = rs_place(k)
        return remote(src, bufs[b].at[i, :, pl.ds(c, hi - lo)], ssem.at[k], rsem.at[k], nbr[a])

    def finish(block):
        for unit in BLOCKS[block]:
            rows = pl.ds(POS[unit] * UNIT, UNIT)
            for k, (s, h, a, lo, hi) in enumerate(RS_LIST):
                if (s ^ (1 << a), h) == unit:
                    piece(k).wait_recv()
                    b, i, c = rs_place(k)
                    dh[rows, lo:hi] += bufs[b][i, :, c:c + hi - lo]
            for k, (s, h, a, lo, hi) in enumerate(RS_LIST):
                if (s, h) == unit:
                    piece(k).start()

    def place(q):
        return NB - 1 - lax.div(q, NT), pl.multiple_of(lax.rem(q, NT) * VT, VT)

    def sdot(q):
        blk, off = place(q)
        return dot_last(e_v[pl.ds(off, VT), :], hn_s[pl.ds(pl.multiple_of(blk * TB, TB), TB), :])

    iota = lax.broadcasted_iota(jnp.int32, (VT, TB), 0)

    def g_copy(i, k):
        blk, off = place(2 * i + k)
        at = 2 * lax.rem(i, 2) + k
        return pltpu.make_async_copy(g_s.at[at], g_ref.at[pl.ds(off, VT), pl.ds(pl.multiple_of(blk * TB, TB), TB)], gsem.at[at])

    def proc(i, k, s):
        blk, off = place(2 * i + k)
        mask_pads(s, lax.rem(2 * i + k, NT))
        w = s[...] - lse_ref[blk]
        hit = iota == (lab_ref[blk] - off)
        p = jnp.exp2(w * LOG2E - 13.0)
        gv = (p - jnp.where(hit, 2.0 ** -13, 0.0)).astype(BF)
        l_ref[...] += jnp.where(hit, w, 0.0).reshape(VT // 8, 8, TB).sum(0)
        g_s[2 * lax.rem(i, 2) + k] = gv
        rows = pl.ds(pl.multiple_of(blk * TB, TB), TB)
        dh[rows, :] += dot_first(gv, e_v[pl.ds(off, VT), :])

    load_e.wait()
    load_h.wait()
    s0[...] = sdot(0)

    def body(i, carry):
        @pl.when(i >= 2)
        def _():
            g_copy(i - 2, 0).wait()
            g_copy(i - 2, 1).wait()
        s1[...] = sdot(2 * i + 1)
        proc(i, 0, s0)
        s0[...] = sdot(jnp.minimum(2 * i + 2, NQ - 1))
        proc(i, 1, s1)
        g_copy(i, 0).start()
        g_copy(i, 1).start()
        for b in range(NB):
            @pl.when(i == (b * NT + NT - 1) // 2)
            def _(b=b):
                finish(NB - 1 - b)
        return carry

    lax.fori_loop(0, NQ // 2, body, 0)
    for i in (NQ // 2 - 2, NQ // 2 - 1):
        g_copy(i, 0).wait()
        g_copy(i, 1).wait()
    dh_ref[...] = dh[pl.ds(0, TOK), :]
    for k in range(len(RS_LIST)):
        piece(k).wait_send()


def head_backward(hn_all, e_loc, lse, lab):
    n = len(RS_LIST)
    return pl.pallas_call(
        bwd_kernel, in_specs=[ANY, ANY, VMEM, VMEM], out_specs=[VMEM, ANY, VMEM],
        out_shape=[jax.ShapeDtypeStruct((TOK, D), F32), jax.ShapeDtypeStruct((VP, GT), BF), jax.ShapeDtypeStruct((8, TB), F32)],
        scratch_shapes=[pltpu.VMEM((VP, D), BF), pltpu.VMEM((GT, D), BF), pltpu.VMEM((VT, TB), F32), pltpu.VMEM((VT, TB), F32),
                        pltpu.VMEM((4, VT, TB), BF), pltpu.VMEM((GT, D), F32),
                        pltpu.VMEM((6, UNIT, 256), F32), pltpu.VMEM((6, UNIT, D), F32), pltpu.VMEM((6, UNIT, D), F32),
                        pltpu.SemaphoreType.DMA((2,)), pltpu.SemaphoreType.DMA((4,)),
                        pltpu.SemaphoreType.DMA((n,)), pltpu.SemaphoreType.DMA((n,))],
        compiler_params=params(2), name='head_bwd')(hn_all, e_loc, lse, lab)


DE_T = 640


def de_kernel(scale, g_ref, hn_ref, rows_ref, dx_ref, out_ref):
    out_ref[...] = dot_plain(g_ref[...], hn_ref[...])
    base = pl.program_id(0) * DE_T
    iota = lax.broadcasted_iota(jnp.int32, (DE_T, NB * CAP), 0)
    pick = jnp.where(iota == rows_ref[...] - base, 1.0, 0.0).astype(BF)
    out_ref[...] += dot_plain(pick, dx_ref[...]) * scale


def embed_grad(g, hn_all, rows, dx, scale):
    n = NB * CAP
    return pl.pallas_call(
        functools.partial(de_kernel, scale), grid=(VP // DE_T,),
        in_specs=[pl.BlockSpec((DE_T, GT), lambda j: (j, 0)), pl.BlockSpec((GT, D), lambda j: (0, 0)),
                  pl.BlockSpec((1, n), lambda j: (0, 0)), pl.BlockSpec((n, D), lambda j: (0, 0))],
        out_specs=pl.BlockSpec((DE_T, D), lambda j: (j, 0)), out_shape=jax.ShapeDtypeStruct((VP, D), F32),
        compiler_params=pltpu.CompilerParams(vmem_limit_bytes=60 * 2 ** 20),
        cost_estimate=pl.CostEstimate(flops=2 * VP * (GT + n) * D, bytes_accessed=VP * GT * 2 + VP * D * 4, transcendentals=0),
        name='embed_grad')(g, hn_all, rows, dx)


def rms_inv(values):
    return lax.rsqrt(jnp.mean(values * values, axis=-1, keepdims=True) + NORM_EPS)


def rms_backward(values, inv_rms, gain_vec, grad_out):
    scaled = grad_out * gain_vec
    return inv_rms * scaled - values * (inv_rms ** 3) * jnp.mean(scaled * values, axis=-1, keepdims=True)


FT = 768
NF = FF // FT


def mlp_fwd_kernel(x_ref, gm_ref, gf_ref, wgu_ref, wd_ref, a_ref, gu_ref, q_ref, h_ref, hn_ref, acc):
    f = pl.program_id(0)

    @pl.when(f == 0)
    def _():
        x = x_ref[...].astype(F32) * EMB_SCALE
        a_ref[...] = (x * rms_inv(x) * gm_ref[...]).astype(BF)
        acc[...] = jnp.zeros_like(acc)
    gu = dot_plain(a_ref[...], wgu_ref[...]).astype(BF)
    gu_ref[...] = gu
    g, u = gu[:, :FT].astype(F32), gu[:, FT:].astype(F32)
    q = (g * jax.nn.sigmoid(g) * u).astype(BF)
    q_ref[...] = q
    acc[...] += dot_plain(q, wd_ref[...])

    @pl.when(f == NF - 1)
    def _():
        x = x_ref[...].astype(F32) * EMB_SCALE
        h = (x + acc[...].astype(BF).astype(F32)).astype(BF)
        h_ref[...] = h
        h = h.astype(F32)
        hn_ref[...] = (h * rms_inv(h) * gf_ref[...]).astype(BF)


def whole(shape):
    return pl.BlockSpec(shape, lambda f: (0, 0))


def mlp_forward(x, gain_mlp, gain_final, w_gu, w_down):
    tok = jax.ShapeDtypeStruct((TOK, D), BF)
    return pl.pallas_call(
        mlp_fwd_kernel, grid=(NF,),
        in_specs=[whole((TOK, D)), whole((1, D)), whole((1, D)), pl.BlockSpec((D, 2 * FT), lambda f: (0, f)),
                  pl.BlockSpec((FT, D), lambda f: (f, 0))],
        out_specs=[whole((TOK, D)), pl.BlockSpec((TOK, 2 * FT), lambda f: (0, f)), pl.BlockSpec((TOK, FT), lambda f: (0, f)),
                   whole((TOK, D)), whole((TOK, D))],
        out_shape=[tok, jax.ShapeDtypeStruct((TOK, 2 * FF), BF), jax.ShapeDtypeStruct((TOK, FF), BF), tok, tok],
        scratch_shapes=[pltpu.VMEM((TOK, D), F32)],
        compiler_params=pltpu.CompilerParams(vmem_limit_bytes=40 * 2 ** 20), name='mlp_fwd')(x, gain_mlp, gain_final, w_gu, w_down)


def mlp_bwd_kernel(dh_ref, h_ref, x_ref, a_ref, gu_ref, q_ref, gm_ref, gf_ref, wgu_ref, wd_ref,
                   dd_ref, dgu_ref, dx_ref, dh_s, dm_s, dn):
    f = pl.program_id(0)

    @pl.when(f == 0)
    def _():
        h = h_ref[...].astype(F32)
        dh = rms_backward(h, rms_inv(h), gf_ref[...], dh_ref[...])
        dh_s[...] = dh
        dm_s[...] = dh.astype(BF)
        dn[...] = jnp.zeros_like(dn)
    dm = dm_s[...]
    dd_ref[...] = dot_first(q_ref[...], dm)
    dq = dot_last(dm, wd_ref[...])
    g, u = gu_ref[:, :FT].astype(F32), gu_ref[:, FT:].astype(F32)
    sig = jax.nn.sigmoid(g)
    dg = (dq * u * sig * (1.0 + g * (1.0 - sig))).astype(BF)
    du = (dq * g * sig).astype(BF)
    a = a_ref[...]
    dgu_ref[:, :FT] = dot_first(a, dg)
    dgu_ref[:, FT:] = dot_first(a, du)
    dn[...] += dot_last(dg, wgu_ref[:, :FT]) + dot_last(du, wgu_ref[:, FT:])

    @pl.when(f == NF - 1)
    def _():
        x = x_ref[...].astype(F32) * EMB_SCALE
        dx_ref[...] = (dh_s[...] + rms_backward(x, rms_inv(x), gm_ref[...], dn[...])).astype(BF)


def mlp_backward(d_hid, h, x, a, gu, q, gain_mlp, gain_final, w_gu, w_down):
    return pl.pallas_call(
        mlp_bwd_kernel, grid=(NF,),
        in_specs=[whole((TOK, D)), whole((TOK, D)), whole((TOK, D)), whole((TOK, D)), pl.BlockSpec((TOK, 2 * FT), lambda f: (0, f)),
                  pl.BlockSpec((TOK, FT), lambda f: (0, f)), whole((1, D)), whole((1, D)),
                  pl.BlockSpec((D, 2 * FT), lambda f: (0, f)), pl.BlockSpec((FT, D), lambda f: (f, 0))],
        out_specs=[pl.BlockSpec((FT, D), lambda f: (f, 0)), pl.BlockSpec((D, 2 * FT), lambda f: (0, f)), whole((TOK, D))],
        out_shape=[jax.ShapeDtypeStruct((FF, D), F32), jax.ShapeDtypeStruct((D, 2 * FF), F32), jax.ShapeDtypeStruct((TOK, D), BF)],
        scratch_shapes=[pltpu.VMEM((TOK, D), F32), pltpu.VMEM((TOK, D), BF), pltpu.VMEM((TOK, D), F32)],
        compiler_params=pltpu.CompilerParams(vmem_limit_bytes=60 * 2 ** 20),
        name='mlp_bwd')(d_hid, h, x, a, gu, q, gain_mlp, gain_final, w_gu, w_down)


def join_parts(gate, up):
    return jnp.concatenate([w[:, f * FT:(f + 1) * FT] for f in range(NF) for w in (gate, up)], 1)


def solution(mesh):
    def local_step(ids_blk, lab_blk, emb_shard, gate_shard, up_shard, down_shard, gain_mlp, gain_final):
        me = lax.axis_index('fsdp')
        core, chip = me % 2, me // 2
        both = lax.all_gather(jnp.concatenate([ids_blk, lab_blk]), 'fsdp')
        w_gu = lax.all_gather(join_parts(gate_shard, up_shard), 'fsdp', tiled=True)
        w_down = lax.all_gather(down_shard, 'fsdp', tiled=True)
        e_loc = pair_gather(emb_shard)

        rel = jnp.stack([peer_of(me, r) for r in range(NB)])
        grp = jnp.take(both, rel, axis=0)
        ids, labs = grp[:, 0], grp[:, 1]

        def local_row(v):
            within = v % (2 * SHARD)
            row = jnp.where(within // SHARD == core, 0, HALF) + within % SHARD
            return jnp.where(v // (2 * SHARD) == chip, row, -1)

        rows = local_row(ids)
        lab_row = local_row(labs)
        mine = (rows >= 0).astype(F32)
        before = (jnp.arange(TOK)[:, None] < jnp.arange(TOK)[None, :]).astype(F32)
        rank = dot_plain(mine, before).astype(jnp.int32)
        slots = jnp.arange(CAP, dtype=jnp.int32)
        own_chip = ids[0] // (2 * SHARD)
        own_rel = jnp.bitwise_xor(own_chip, chip)
        is_rel = own_rel[None, :] == jnp.arange(NB)[:, None]
        own_rank_all = dot_plain(is_rel.astype(F32), before)
        own_rank = jnp.sum(jnp.where(is_rel, own_rank_all, 0.0), 0).astype(jnp.int32)
        counts = jnp.sum((both[:, 0] // (2 * SHARD))[:, None, :] == jnp.arange(NB)[None, :, None], axis=-1)
        rounds = (jnp.max(counts) + CAP - 1) // CAP

        def slot_rows(rnd):
            want = (rows[:, None, :] >= 0) & (rank[:, None, :] - rnd * CAP == slots[None, :, None])
            got = jnp.sum(jnp.where(want, rows[:, None, :] + 1, 0), axis=-1) - 1
            return got.reshape(NB * CAP)

        def slot_tokens(rnd):
            want = is_rel[:, None, :] & (own_rank[None, None, :] - rnd * CAP == slots[None, :, None])
            return jnp.sum(jnp.where(want, jnp.arange(TOK)[None, None, :], 0), axis=-1).reshape(NB * CAP)

        def lookup(rnd, x, cid):
            out = jnp.take(e_loc, jnp.maximum(slot_rows(rnd), 0), axis=0, mode='clip').reshape(NB, CAP, D)
            got = swap(out, cid).reshape(NB * CAP, D)
            here = own_rank // CAP == rnd
            at = jnp.where(here, own_rel * CAP + own_rank % CAP, 0)
            return jnp.where(here[:, None], jnp.take(got, at, axis=0, mode='clip'), x)

        x_bf = lookup(0, jnp.zeros((TOK, D), BF), 3)
        x_bf = lax.while_loop(lambda c: c[0] < rounds, lambda c: (c[0] + 1, lookup(c[0], c[1], 4)), (jnp.int32(1), x_bf))[1]

        gm, gf = gain_mlp[None, :], gain_final[None, :]
        normed, gu, hidden_act, hid, hid_norm = mlp_forward(x_bf, gm, gf, w_gu, w_down)

        hn_all, lse = head_forward(hid_norm, e_loc)
        lab_pos = jnp.concatenate([lab_row[r, h * UNIT:(h + 1) * UNIT] for r, h in UNITS]).reshape(NB, 1, TB)
        d_hid, g_all, loss8 = head_backward(hn_all, e_loc, lse, lab_pos)
        loss = lax.psum(-jnp.sum(loss8), 'fsdp') * (1.0 / TOTAL)

        d_down, d_gu, d_x = mlp_backward(d_hid, hid, x_bf, normed, gu, hidden_act, gm, gf, w_gu, w_down)
        d_down = lax.psum_scatter(d_down, 'fsdp', scatter_dimension=0, tiled=True)
        d_gu = lax.psum_scatter(d_gu, 'fsdp', scatter_dimension=0, tiled=True)

        def send_dx(rnd, cid):
            return swap(jnp.take(d_x, slot_tokens(rnd), axis=0, mode='clip').reshape(NB, CAP, D), cid).reshape(NB * CAP, D)

        d_loc = embed_grad(g_all, hn_all, slot_rows(0)[None, :], send_dx(0, 5), EMB_SCALE)

        def more(c):
            rnd, acc = c
            at = slot_rows(rnd)
            add = jnp.where((at >= 0)[:, None], send_dx(rnd, 6).astype(F32) * EMB_SCALE, 0.0)
            return rnd + 1, acc.at[jnp.maximum(at, 0)].add(add)

        d_loc = lax.while_loop(lambda c: c[0] < rounds, more, (jnp.int32(1), d_loc))[1]
        pairs = [(d, d ^ 1) for d in range(2 * NB)]
        d_embed = d_loc[:SHARD] + lax.ppermute(d_loc[HALF:HALF + SHARD], 'fsdp', pairs)
        d_gu = d_gu.reshape(-1, NF, 2, FT)
        return loss, d_embed, d_gu[:, :, 0].reshape(-1, FF), d_gu[:, :, 1].reshape(-1, FF), d_down

    shard = P('fsdp', None)
    return jax.shard_map(local_step, mesh=mesh, in_specs=(shard,) * 6 + (P(), P()),
                         out_specs=(P(), shard, shard, shard, shard), check_vma=False)
```

```python
import functools
import math
import jax
import jax.numpy as jnp
from jax import lax
from jax.experimental import pallas as pl
from jax.experimental.pallas import tpu as pltpu
from jax.sharding import PartitionSpec as P

NORM_EPS = 1e-6
LOG2E = 1.4426950408889634
MESH = pl.DeviceIdType.MESH
ANY = pl.BlockSpec(memory_space=pl.ANY)
VMEM = pl.BlockSpec(memory_space=pltpu.VMEM)
BF = jnp.bfloat16
F32 = jnp.float32
DMA = pltpu.SemaphoreType.DMA

SHARD = 3144
HALF = 3200
VP = 2 * HALF
D = 768
FF = 3072
TOK = 512
UNIT = 256
NB = 8
TB = 512
GT = NB * TOK
VT = 1280
NT = VP // VT
NQ = NB * NT
CAP = 96
SLOTS = NB * CAP
TOTAL = 8192
NDEV = 2 * NB
CHIP_ROWS = 2 * SHARD
FF2 = 2 * FF
EMB_SCALE = math.sqrt(D)

CUBE = range(NB)
AXES = range(3)
HALVES = range(2)


def unit_list(text):
    return [(int(r), 'ab'.index(h)) for r, h in zip(text[::2], text[1::2])]


UNITS = unit_list('0a0b2b1b4b1a4a2a3b6b5b3a6a5a7a7b')
BLOCKS = list(zip(UNITS[::2], UNITS[1::2]))
POS = {u: i for i, u in enumerate(UNITS)}
WAITS = {1: '2b1b4b', 2: '1a4a2a', 4: '3b6b5b', 5: '3a6a5a', 7: '7a7b'}
ROW, COL = D // 3, D // 2
CORNER = NB - 1
STAR = [(1 << a, a, 0, D) for a in AXES]
EDGE = [(CORNER - (1 << b), (b + 1 + j) % 3, j * COL, (j + 1) * COL) for b in (1, 0, 2) for j in HALVES]
TIP = [(CORNER, a, a * ROW, (a + 1) * ROW) for a in AXES]
SUMS = TIP + EDGE + STAR


def landing(path):
    s, a, lo, hi = path
    t = s - (1 << a)
    if s == CORNER:
        return 0, a, 0
    return (1, STAR_AT[t], lo) if t else (2, a, 0)


STAR_AT = {1 << a: a for a in AXES}


def dot_plain(a, b):
    return lax.dot_general(a, b, (((1,), (0,)), ((), ())), preferred_element_type=F32)


def dot_last(a, b):
    return lax.dot_general(a, b, (((1,), (1,)), ((), ())), preferred_element_type=F32)


def dot_first(a, b):
    return lax.dot_general(a, b, (((0,), (0,)), ((), ())), preferred_element_type=F32)


def peer_of(me, r):
    p = me
    for a in AXES:
        if r >> a & 1:
            step = 2 << a
            p = p + step - step * (me // step % 2 * 2)
    return p


def barrier_with(peers):
    sem = pltpu.get_barrier_semaphore()
    for p in peers:
        pl.semaphore_signal(sem, inc=1, device_id=(p,), device_id_type=MESH)
    pl.semaphore_wait(sem, len(peers))


def remote(src, dst, ssem, rsem, dev):
    return pltpu.make_async_remote_copy(src_ref=src, dst_ref=dst, send_sem=ssem, recv_sem=rsem,
                                        device_id=(dev,), device_id_type=MESH)


def params(cid, mib=60):
    return pltpu.CompilerParams(collective_id=cid, has_side_effects=True, vmem_limit_bytes=mib * 2 ** 20)


def pair_kernel(e_ref, out_ref, buf, zero, sems, ssem, rsem):
    me = lax.axis_index('fsdp')
    other = me + 1 - 2 * (me % 2)
    barrier_with([other])
    load = pltpu.make_async_copy(e_ref, buf, sems.at[0])
    load.start()
    zero[...] = jnp.zeros_like(zero)
    load.wait()
    send = remote(buf, out_ref.at[pl.ds(HALF, SHARD)], ssem, rsem, other)
    send.start()
    copies = [pltpu.make_async_copy(buf, out_ref.at[pl.ds(0, SHARD)], sems.at[1]),
              pltpu.make_async_copy(zero, out_ref.at[pl.ds(SHARD, HALF - SHARD)], sems.at[2]),
              pltpu.make_async_copy(zero, out_ref.at[pl.ds(HALF + SHARD, HALF - SHARD)], sems.at[3])]
    for c in copies:
        c.start()
    for c in copies:
        c.wait()
    send.wait()


def pair_gather(e_shard):
    return pl.pallas_call(
        pair_kernel, in_specs=[ANY], out_specs=ANY, out_shape=jax.ShapeDtypeStruct((VP, D), BF),
        scratch_shapes=[pltpu.VMEM((SHARD, D), BF), pltpu.VMEM((HALF - SHARD, D), BF), DMA((4,)),
                        DMA, DMA],
        compiler_params=params(0, 16), name='pair_gather')(e_shard)


def swap_kernel(in_ref, out_ref, recv, ssem, rsem):
    me = lax.axis_index('fsdp')
    peers = [peer_of(me, r) for r in range(1, NB)]
    barrier_with(peers)
    sends = [remote(in_ref.at[r], recv.at[r], ssem.at[r], rsem.at[r], peers[r - 1]) for r in range(1, NB)]
    for s in sends:
        s.start()
    out_ref[0] = in_ref[0]
    for r in range(1, NB):
        sends[r - 1].wait()
        out_ref[r] = recv[r]


def swap(rows, cid):
    return pl.pallas_call(
        swap_kernel, in_specs=[VMEM], out_specs=VMEM, out_shape=jax.ShapeDtypeStruct((NB, CAP, D), BF),
        scratch_shapes=[pltpu.VMEM((NB, CAP, D), BF), DMA((NB,)), DMA((NB,))],
        compiler_params=params(cid, 16), name='swap')(rows)


def mask_pads(s, j):
    for tile, at in ((2, SHARD - 2 * VT), (4, HALF + SHARD - 4 * VT)):
        rows = pl.ds(at, HALF - SHARD)
        s[rows, :] = jnp.where(j == tile, -jnp.inf, s[rows, :])


AG_PATHS = [(0, a, 0, D) for a in AXES] + [(1 << (a + 1) % 3, a, 0, D) for a in AXES] + [(CORNER - (1 << a), a, lo, hi) for _, a, lo, hi in TIP]
AG_LIST = [(s, h, a, lo, hi) for h in (1, 0) for (s, a, lo, hi) in AG_PATHS]


def fwd_kernel(hn_ref, e_ref, all_ref, lse_ref, e_v, hn_s, s0, s1, st, stat, csem, ssem, rsem, ssem2, rsem2):
    me = lax.axis_index('fsdp')
    nbr = [peer_of(me, 1 << a) for a in range(3)]
    peers = [peer_of(me, r) for r in range(1, NB)]
    barrier_with(peers)
    load_e = pltpu.make_async_copy(e_ref, e_v, csem.at[0])
    load_e.start()
    load_h = pltpu.make_async_copy(hn_ref, hn_s.at[pl.ds(0, TOK)], csem.at[1])
    load_h.start()
    load_h.wait()

    def piece(k):
        s, h, a, lo, hi = AG_LIST[k]
        src = hn_s.at[pl.ds(POS[(s, h)] * UNIT, UNIT), pl.ds(lo, hi - lo)]
        dst = hn_s.at[pl.ds(POS[(s ^ (1 << a), h)] * UNIT, UNIT), pl.ds(lo, hi - lo)]
        return remote(src, dst, ssem.at[k], rsem.at[k], nbr[a])

    def forward(unit):
        for k, (s, h, a, lo, hi) in enumerate(AG_LIST):
            if (s, h) == unit:
                piece(k).start()

    def arrive(units):
        for unit in units:
            for k, (s, h, a, lo, hi) in enumerate(AG_LIST):
                if (s ^ (1 << a), h) == unit:
                    piece(k).wait_recv()
            forward(unit)

    forward((0, 1))
    forward((0, 0))
    st[:, 0] = jnp.full((NB, 8, TB), -jnp.inf, F32)
    st[:, 1] = jnp.zeros((NB, 8, TB), F32)
    load_e.wait()

    def sdot(q):
        off = pl.multiple_of(lax.rem(q, NT) * VT, VT)
        tok = pl.multiple_of(lax.div(q, NT) * TB, TB)
        return dot_last(e_v[pl.ds(off, VT), :], hn_s[pl.ds(tok, TB), :])

    def proc(q, s):
        blk = lax.div(q, NT)
        s3 = s[...].reshape(VT // 8, 8, TB)
        m8 = st[blk, 0]
        nm = jnp.maximum(m8, s3.max(0))
        st[blk, 1] = st[blk, 1] * jnp.exp2((m8 - nm) * LOG2E) + jnp.exp2((s3 - nm[None]) * LOG2E).sum(0)
        st[blk, 0] = nm

    s0[...] = sdot(0)

    def body(i, carry):
        q = 2 * i
        for block, units in WAITS.items():
            @pl.when(i == (block * NT - 1) // 2)
            def _(units=units):
                arrive(unit_list(units))
        s1[...] = sdot(q + 1)
        mask_pads(s0, lax.rem(q, NT))
        proc(q, s0)
        s0[...] = sdot(jnp.minimum(q + 2, NQ - 1))
        mask_pads(s1, lax.rem(q + 1, NT))
        proc(q + 1, s1)
        return carry

    lax.fori_loop(0, NQ // 2, body, 0)
    out = pltpu.make_async_copy(hn_s, all_ref, csem.at[2])
    out.start()

    def unit_stat(unit):
        blk, at = POS[unit] // 2, (POS[unit] % 2) * UNIT
        m8, s8 = st[blk, 0, :, at:at + UNIT], st[blk, 1, :, at:at + UNIT]
        m = m8.max(0, keepdims=True)
        return m, (s8 * jnp.exp2((m8 - m) * LOG2E)).sum(0, keepdims=True)

    def stat_at(k, r):
        return stat.at[k, k ^ r, 0:1], stat.at[k, k ^ r, 1:2]

    for r in CUBE:
        for h in HALVES:
            for ref, val in zip(stat_at(0, r), unit_stat((r, h))):
                ref[:, h * UNIT:(h + 1) * UNIT] = val
    sends = [remote(stat.at[0], stat.at[r], ssem2.at[r], rsem2.at[r], peers[r - 1]) for r in range(1, NB)]
    for c in sends:
        c.start()
    for c in sends:
        c.wait()
    for r in CUBE:
        parts = [stat_at(k, r) for k in CUBE]
        top = functools.reduce(jnp.maximum, [m[...] for m, _ in parts])
        lse = top + jnp.log(sum(s[...] * jnp.exp2((m[...] - top) * LOG2E) for m, s in parts))
        for h in HALVES:
            blk, at = POS[(r, h)] // 2, (POS[(r, h)] % 2) * UNIT
            lse_ref[blk, :, at:at + UNIT] = lse[:, h * UNIT:(h + 1) * UNIT]
    for k in range(len(AG_LIST)):
        piece(k).wait_send()
    out.wait()


def head_forward(hn, e_loc):
    n = len(AG_LIST)
    return pl.pallas_call(
        fwd_kernel, in_specs=[ANY, ANY], out_specs=[ANY, VMEM],
        out_shape=[jax.ShapeDtypeStruct((GT, D), BF), jax.ShapeDtypeStruct((NB, 1, TB), F32)],
        scratch_shapes=[pltpu.VMEM((VP, D), BF), pltpu.VMEM((GT, D), BF), pltpu.VMEM((VT, TB), F32), pltpu.VMEM((VT, TB), F32),
                        pltpu.VMEM((NB, 2, 8, TB), F32), pltpu.VMEM((NB, NB, 2, TB), F32), DMA((3,)),
                        DMA((n,)), DMA((n,)),
                        DMA((NB,)), DMA((NB,))],
        compiler_params=params(1), name='head_fwd')(hn, e_loc)


RS_LIST = [(p, h) for p in SUMS for h in HALVES]


def bwd_kernel(hn_ref, e_ref, lse_ref, lab_ref, dh_ref, g_ref, l_ref,
               e_v, hn_s, s0, s1, g_s, dh, ra, rb, rc, csem, gsem, ssem, rsem):
    me = lax.axis_index('fsdp')
    nbr = [peer_of(me, 1 << a) for a in range(3)]
    barrier_with(nbr)
    load_e = pltpu.make_async_copy(e_ref, e_v, csem.at[0])
    load_e.start()
    load_h = pltpu.make_async_copy(hn_ref, hn_s, csem.at[1])
    load_h.start()
    dh[...] = jnp.zeros_like(dh)
    l_ref[...] = jnp.zeros_like(l_ref)
    bufs = (ra, rb, rc)

    def piece(k):
        (s, a, lo, hi), h = RS_LIST[k]
        src = dh.at[pl.ds(POS[(s, h)] * UNIT, UNIT), pl.ds(lo, hi - lo)]
        b, i, c = landing(RS_LIST[k][0])
        return remote(src, bufs[b].at[2 * i + h, :, pl.ds(c, hi - lo)], ssem.at[k], rsem.at[k], nbr[a])

    def finish(block):
        for r, half in BLOCKS[block]:
            rows = pl.ds(POS[(r, half)] * UNIT, UNIT)
            for k, (path, h) in enumerate(RS_LIST):
                s, a, lo, hi = path
                if (s ^ (1 << a), h) == (r, half):
                    piece(k).wait_recv()
                    b, i, c = landing(path)
                    dh[rows, lo:hi] += bufs[b][2 * i + h, :, c:c + hi - lo]
            for k, (path, h) in enumerate(RS_LIST):
                if (path[0], h) == (r, half):
                    piece(k).start()

    def place(q):
        return NB - 1 - lax.div(q, NT), pl.multiple_of(lax.rem(q, NT) * VT, VT)

    def sdot(q):
        blk, off = place(q)
        return dot_last(e_v[pl.ds(off, VT), :], hn_s[pl.ds(pl.multiple_of(blk * TB, TB), TB), :])

    iota = lax.broadcasted_iota(jnp.int32, (VT, TB), 0)

    def g_copy(i, k):
        blk, off = place(2 * i + k)
        at = 2 * lax.rem(i, 2) + k
        return pltpu.make_async_copy(g_s.at[at], g_ref.at[pl.ds(off, VT), pl.ds(pl.multiple_of(blk * TB, TB), TB)], gsem.at[at])

    def proc(i, k, s):
        blk, off = place(2 * i + k)
        mask_pads(s, lax.rem(2 * i + k, NT))
        w = s[...] - lse_ref[blk]
        hit = iota == (lab_ref[blk] - off)
        p = jnp.exp2(w * LOG2E - 13.0)
        gv = (p - jnp.where(hit, 2.0 ** -13, 0.0)).astype(BF)
        l_ref[...] += jnp.where(hit, w, 0.0).reshape(VT // 8, 8, TB).sum(0)
        g_s[2 * lax.rem(i, 2) + k] = gv
        rows = pl.ds(pl.multiple_of(blk * TB, TB), TB)
        dh[rows, :] += dot_first(gv, e_v[pl.ds(off, VT), :])

    load_e.wait()
    load_h.wait()
    s0[...] = sdot(0)

    def body(i, carry):
        @pl.when(i >= 2)
        def _():
            g_copy(i - 2, 0).wait()
            g_copy(i - 2, 1).wait()
        s1[...] = sdot(2 * i + 1)
        proc(i, 0, s0)
        s0[...] = sdot(jnp.minimum(2 * i + 2, NQ - 1))
        proc(i, 1, s1)
        g_copy(i, 0).start()
        g_copy(i, 1).start()
        for b in range(NB):
            @pl.when(i == (b * NT + NT - 1) // 2)
            def _(b=b):
                finish(NB - 1 - b)
        return carry

    lax.fori_loop(0, NQ // 2, body, 0)
    for i in (NQ // 2 - 2, NQ // 2 - 1):
        g_copy(i, 0).wait()
        g_copy(i, 1).wait()
    dh_ref[...] = dh[pl.ds(0, TOK), :]
    for k in range(len(RS_LIST)):
        piece(k).wait_send()


def head_backward(hn_all, e_loc, lse, lab):
    n = len(RS_LIST)
    return pl.pallas_call(
        bwd_kernel, in_specs=[ANY, ANY, VMEM, VMEM], out_specs=[VMEM, ANY, VMEM],
        out_shape=[jax.ShapeDtypeStruct((TOK, D), F32), jax.ShapeDtypeStruct((VP, GT), BF), jax.ShapeDtypeStruct((8, TB), F32)],
        scratch_shapes=[pltpu.VMEM((VP, D), BF), pltpu.VMEM((GT, D), BF), pltpu.VMEM((VT, TB), F32), pltpu.VMEM((VT, TB), F32),
                        pltpu.VMEM((4, VT, TB), BF), pltpu.VMEM((GT, D), F32),
                        pltpu.VMEM((6, UNIT, 256), F32), pltpu.VMEM((6, UNIT, D), F32), pltpu.VMEM((6, UNIT, D), F32),
                        DMA((2,)), DMA((4,)),
                        DMA((n,)), DMA((n,))],
        compiler_params=params(2), name='head_bwd')(hn_all, e_loc, lse, lab)


ET = 320
HT = HALF // ET
NE = 2 * HT
GD_ROWS = FF // (NDEV)
GU_ROWS = D // (NDEV)
SUM_ORDER = [CORNER] + [p[0] for p in EDGE[::2] + STAR[::-1]] + [0]


def last_kernel(dd_ref, dgu_ref, dxs_ref, rows_ref, g_ref, hn_ref, l_ref,
                de_ref, ogu_ref, odd_ref, loss_ref, pe_ref,
                acc_d, acc_g, pair_d, pair_g, ra_d, ra_g, rb_d, rb_g, rc_d, rc_g, dxr, hn_s, g_s, ob, pb, lbuf,
                psem, qsem, lsem, ssem, rsem, xs, xr, es, er, gsem, osem, csem, ls, lr):
    me = lax.axis_index('fsdp')
    core = me % 2
    other = me + 1 - 2 * core
    peers = [peer_of(me, r) for r in range(NB)]
    far = [peers[r] + 1 - 2 * core for r in range(NB)]
    everyone = peers[1:] + far
    barrier_with(everyone)

    lbuf[me] = sum(l_ref[:, k * 128:(k + 1) * 128] for k in range(TB // 128))
    mats = ((dd_ref, acc_d, pair_d, GD_ROWS), (dgu_ref, acc_g, pair_g, GU_ROWS))

    def pair_copy(r, m):
        src, _, dst, n = mats[m]
        return remote(src.at[pl.ds(pl.multiple_of(far[r] * n, n), n)], dst.at[r], psem.at[r, m], qsem.at[r, m], other)

    def own_copy(r, m):
        src, dst, _, n = mats[m]
        return pltpu.make_async_copy(src.at[pl.ds(pl.multiple_of(peers[r] * n, n), n)], dst.at[r], lsem.at[r, m])

    for r in SUM_ORDER:
        for m in range(2):
            pair_copy(r, m).start()
            own_copy(r, m).start()
    dx_copies = [remote(dxs_ref.at[pl.ds(r * CAP, CAP)], dxr.at[pl.ds(r * CAP, CAP)], xs.at[r], xr.at[r], peers[r])
                 for r in range(1, NB)]
    for c in dx_copies:
        c.start()
    loss_copies = [remote(lbuf.at[me], lbuf.at[me], ls.at[i], lr.at[i], p) for i, p in enumerate(everyone)]
    for c in loss_copies:
        c.start()
    dx_own = pltpu.make_async_copy(dxs_ref.at[pl.ds(0, CAP)], dxr.at[pl.ds(0, CAP)], csem.at[0])
    dx_own.start()
    load_h = pltpu.make_async_copy(hn_ref, hn_s, csem.at[1])
    load_h.start()

    def odd(t):
        return lax.rem(t, 2)

    def g_load(t):
        off = pl.multiple_of(lax.rem(t + HT, NE) * ET, ET)
        return pltpu.make_async_copy(g_ref.at[pl.ds(off, ET)], g_s.at[odd(t)], gsem.at[odd(t)])

    g_load(0).start()
    bufs = ((ra_d, ra_g), (rb_d, rb_g), (rc_d, rc_g))
    accs = (acc_d, acc_g)

    def piece(k, m):
        s, a, lo, hi = SUMS[k]
        w = (1, 8)[m]
        b, i, c = landing(SUMS[k])
        return remote(accs[m].at[s, :, pl.ds(lo * w, (hi - lo) * w)], bufs[b][m].at[i, :, pl.ds(c * w, (hi - lo) * w)],
                      ssem.at[k, m], rsem.at[k, m], peers[1 << a])

    def pair_sum(r):
        for m in range(2):
            own_copy(r, m).wait()
            pair_copy(r, m).wait_recv()
            accs[m][r] += mats[m][2][r]

    def pass_on(r):
        for m in range(2):
            w = (1, 8)[m]
            for k, (s, a, lo, hi) in enumerate(SUMS):
                if s ^ (1 << a) == r:
                    piece(k, m).wait_recv()
                    b, i, c = landing(SUMS[k])
                    accs[m][r, :, lo * w:hi * w] += bufs[b][m][i, :, c * w:(c + hi - lo) * w]
            for k, (s, a, lo, hi) in enumerate(SUMS):
                if s == r:
                    piece(k, m).start()

    pair_sum(7)
    pass_on(7)
    for r in SUM_ORDER[1:]:
        pair_sum(r)
    dx_own.wait()
    load_h.wait()
    for c in dx_copies:
        c.wait_recv()

    def e_send(t):
        return remote(ob.at[odd(t)], pe_ref.at[pl.ds(pl.multiple_of(t * ET, ET), ET)], es.at[t], er.at[t], other)

    def e_out(t, n=ET):
        at = pl.multiple_of((t - HT) * ET, ET)
        return pltpu.make_async_copy(ob.at[odd(t), pl.ds(0, n)], de_ref.at[pl.ds(at, n)], osem.at[odd(t)])

    def e_load(t):
        return pltpu.make_async_copy(pe_ref.at[pl.ds(pl.multiple_of((t - HT) * ET, ET), ET)], pb, csem.at[2])

    iota = lax.broadcasted_iota(jnp.int32, (ET, SLOTS), 0)
    last = SHARD - (HT - 1) * ET

    def body(t, carry):
        for when, rs in ((5, SUM_ORDER[1:4]), (NE - 3, SUM_ORDER[4:7])):
            @pl.when(t == when)
            def _(rs=rs):
                for r in rs:
                    pass_on(r)

        @pl.when((t >= 2) & (t < HT + 2))
        def _():
            e_send(t - 2).wait_send()

        @pl.when(t >= HT + 2)
        def _():
            e_out(t - 2).wait()

        @pl.when(t >= HT)
        def _():
            e_send(t - HT).wait_recv()
            e_load(t).start()

        @pl.when(t < NE - 1)
        def _():
            g_load(t + 1).start()
        g_load(t).wait()
        base = lax.rem(t + HT, NE) * ET
        pick = jnp.where(iota == rows_ref[...] - base, 1.0, 0.0).astype(BF)
        ob[odd(t)] = dot_plain(g_s[odd(t)], hn_s[...]) + dot_plain(pick, dxr[...]) * EMB_SCALE

        @pl.when(t < HT)
        def _():
            e_send(t).start()

        @pl.when(t >= HT)
        def _():
            e_load(t).wait()
            ob[odd(t)] += pb[...]

        @pl.when((t >= HT) & (t < NE - 1))
        def _():
            e_out(t).start()

        @pl.when(t == NE - 1)
        def _():
            e_out(t, last).start()
        return carry

    lax.fori_loop(0, NE, body, 0)
    for c in loss_copies:
        c.wait()
    tot = lbuf[0]
    for i in range(1, NDEV):
        tot = tot + lbuf[i]
    loss_ref[...] = tot
    pass_on(0)
    ogu_ref[...] = acc_g[0]
    odd_ref[...] = acc_d[0]
    e_out(NE - 2).wait()
    e_out(NE - 1, last).wait()
    for c in dx_copies:
        c.wait_send()
    for m in range(2):
        for r in SUM_ORDER:
            pair_copy(r, m).wait_send()
        for k in range(len(SUMS)):
            piece(k, m).wait_send()


def last_sums(d_down, d_gu, dxs, rows, g_all, hn_all, loss8):
    n = len(SUMS)
    scr = [pltpu.VMEM(s, F32) for s in ((NB, GD_ROWS, D), (NB, GU_ROWS, FF2), (NB, GD_ROWS, D), (NB, GU_ROWS, FF2),
                                        (3, GD_ROWS, 256), (3, GU_ROWS, 2048), (3, GD_ROWS, D), (3, GU_ROWS, FF2),
                                        (3, GD_ROWS, D), (3, GU_ROWS, FF2))]
    scr += [pltpu.VMEM((SLOTS, D), BF), pltpu.VMEM((GT, D), BF), pltpu.VMEM((2, ET, GT), BF), pltpu.VMEM((2, ET, D), F32),
            pltpu.VMEM((ET, D), F32), pltpu.VMEM((NDEV, 8, 128), F32)]
    scr += [DMA((NB, 2)), DMA((NB, 2)), DMA((NB, 2)), DMA((n, 2)), DMA((n, 2)), DMA((NB,)), DMA((NB,)), DMA((HT,)), DMA((HT,)),
            DMA((2,)), DMA((2,)), DMA((3,)), DMA((NDEV - 1,)), DMA((NDEV - 1,))]
    return pl.pallas_call(
        last_kernel, in_specs=[ANY, ANY, ANY, VMEM, ANY, ANY, VMEM], out_specs=[ANY, VMEM, VMEM, VMEM, ANY],
        out_shape=[jax.ShapeDtypeStruct((SHARD, D), F32), jax.ShapeDtypeStruct((GU_ROWS, FF2), F32),
                   jax.ShapeDtypeStruct((GD_ROWS, D), F32), jax.ShapeDtypeStruct((8, 128), F32),
                   jax.ShapeDtypeStruct((HALF, D), F32)],
        scratch_shapes=scr, compiler_params=params(7, 63), name='last_sums')(d_down, d_gu, dxs, rows, g_all, hn_all, loss8)


def rms_inv(values):
    return lax.rsqrt(jnp.mean(values * values, axis=-1, keepdims=True) + NORM_EPS)


def rms_backward(values, inv_rms, gain_vec, grad_out):
    scaled = grad_out * gain_vec
    return inv_rms * scaled - values * (inv_rms ** 3) * jnp.mean(scaled * values, axis=-1, keepdims=True)


FT = 768
FT2 = 2 * FT
NF = FF // FT


def mlp_fwd_kernel(x_ref, gm_ref, gf_ref, wgu_ref, wd_ref, a_ref, gu_ref, q_ref, h_ref, hn_ref, acc):
    f = pl.program_id(0)

    @pl.when(f == 0)
    def _():
        x = x_ref[...].astype(F32) * EMB_SCALE
        a_ref[...] = (x * rms_inv(x) * gm_ref[...]).astype(BF)
        acc[...] = jnp.zeros_like(acc)
    gu = dot_plain(a_ref[...], wgu_ref[...]).astype(BF)
    gu_ref[...] = gu
    g, u = gu[:, :FT].astype(F32), gu[:, FT:].astype(F32)
    q = (g * jax.nn.sigmoid(g) * u).astype(BF)
    q_ref[...] = q
    acc[...] += dot_plain(q, wd_ref[...])

    @pl.when(f == NF - 1)
    def _():
        x = x_ref[...].astype(F32) * EMB_SCALE
        h = (x + acc[...].astype(BF).astype(F32)).astype(BF)
        h_ref[...] = h
        h = h.astype(F32)
        hn_ref[...] = (h * rms_inv(h) * gf_ref[...]).astype(BF)


def whole(shape):
    return pl.BlockSpec(shape, lambda f: (0, 0))


def mlp_forward(x, gain_mlp, gain_final, w_gu, w_down):
    tok = jax.ShapeDtypeStruct((TOK, D), BF)
    return pl.pallas_call(
        mlp_fwd_kernel, grid=(NF,),
        in_specs=[whole((TOK, D)), whole((1, D)), whole((1, D)), pl.BlockSpec((D, FT2), lambda f: (0, f)),
                  pl.BlockSpec((FT, D), lambda f: (f, 0))],
        out_specs=[whole((TOK, D)), pl.BlockSpec((TOK, FT2), lambda f: (0, f)), pl.BlockSpec((TOK, FT), lambda f: (0, f)),
                   whole((TOK, D)), whole((TOK, D))],
        out_shape=[tok, jax.ShapeDtypeStruct((TOK, FF2), BF), jax.ShapeDtypeStruct((TOK, FF), BF), tok, tok],
        scratch_shapes=[pltpu.VMEM((TOK, D), F32)],
        compiler_params=pltpu.CompilerParams(vmem_limit_bytes=40 * 2 ** 20), name='mlp_fwd')(x, gain_mlp, gain_final, w_gu, w_down)


def mlp_bwd_kernel(dh_ref, h_ref, x_ref, a_ref, gu_ref, q_ref, gm_ref, gf_ref, slot_ref, wgu_ref, wd_ref,
                   dd_ref, dgu_ref, dx_ref, dxs_ref, dh_s, dm_s, dn):
    f = pl.program_id(0)

    @pl.when(f == 0)
    def _():
        h = h_ref[...].astype(F32)
        dh = rms_backward(h, rms_inv(h), gf_ref[...], dh_ref[...])
        dh_s[...] = dh
        dm_s[...] = dh.astype(BF)
        dn[...] = jnp.zeros_like(dn)
    dm = dm_s[...]
    dd_ref[...] = dot_first(q_ref[...], dm)
    dq = dot_last(dm, wd_ref[...])
    g, u = gu_ref[:, :FT].astype(F32), gu_ref[:, FT:].astype(F32)
    sig = jax.nn.sigmoid(g)
    dg = (dq * u * sig * (1.0 + g * (1.0 - sig))).astype(BF)
    du = (dq * g * sig).astype(BF)
    a = a_ref[...]
    dgu_ref[:, :FT] = dot_first(a, dg)
    dgu_ref[:, FT:] = dot_first(a, du)
    dn[...] += dot_last(dg, wgu_ref[:, :FT]) + dot_last(du, wgu_ref[:, FT:])

    @pl.when(f == NF - 1)
    def _():
        x = x_ref[...].astype(F32) * EMB_SCALE
        dx = (dh_s[...] + rms_backward(x, rms_inv(x), gm_ref[...], dn[...])).astype(BF)
        dx_ref[...] = dx
        pick = lax.broadcasted_iota(jnp.int32, (SLOTS, TOK), 0) == slot_ref[...]
        dxs_ref[...] = dot_plain(jnp.where(pick, 1.0, 0.0).astype(BF), dx).astype(BF)


def mlp_backward(d_hid, h, x, a, gu, q, gain_mlp, gain_final, slot, w_gu, w_down):
    return pl.pallas_call(
        mlp_bwd_kernel, grid=(NF,),
        in_specs=[whole((TOK, D)), whole((TOK, D)), whole((TOK, D)), whole((TOK, D)), pl.BlockSpec((TOK, FT2), lambda f: (0, f)),
                  pl.BlockSpec((TOK, FT), lambda f: (0, f)), whole((1, D)), whole((1, D)), whole((1, TOK)),
                  pl.BlockSpec((D, FT2), lambda f: (0, f)), pl.BlockSpec((FT, D), lambda f: (f, 0))],
        out_specs=[pl.BlockSpec((FT, D), lambda f: (f, 0)), pl.BlockSpec((D, FT2), lambda f: (0, f)), whole((TOK, D)),
                   whole((SLOTS, D))],
        out_shape=[jax.ShapeDtypeStruct((FF, D), F32), jax.ShapeDtypeStruct((D, FF2), F32), jax.ShapeDtypeStruct((TOK, D), BF),
                   jax.ShapeDtypeStruct((SLOTS, D), BF)],
        scratch_shapes=[pltpu.VMEM((TOK, D), F32), pltpu.VMEM((TOK, D), BF), pltpu.VMEM((TOK, D), F32)],
        compiler_params=pltpu.CompilerParams(vmem_limit_bytes=60 * 2 ** 20),
        name='mlp_bwd')(d_hid, h, x, a, gu, q, gain_mlp, gain_final, slot, w_gu, w_down)


def join_parts(gate, up):
    return jnp.concatenate([w[:, f * FT:(f + 1) * FT] for f in range(NF) for w in (gate, up)], 1)


def solution(mesh):
    def local_step(ids_blk, lab_blk, emb_shard, gate_shard, up_shard, down_shard, gain_mlp, gain_final):
        me = lax.axis_index('fsdp')
        core, chip = me % 2, me // 2
        both = lax.all_gather(jnp.concatenate([ids_blk, lab_blk]), 'fsdp')
        w_gu = lax.all_gather(join_parts(gate_shard, up_shard), 'fsdp', tiled=True)
        w_down = lax.all_gather(down_shard, 'fsdp', tiled=True)
        e_loc = pair_gather(emb_shard)

        rel = jnp.stack([peer_of(me, r) for r in range(NB)])
        grp = jnp.take(both, rel, axis=0)
        ids, labs = grp[:, 0], grp[:, 1]

        def local_row(v):
            within = v % (CHIP_ROWS)
            row = jnp.where(within // SHARD == core, 0, HALF) + within % SHARD
            return jnp.where(v // (CHIP_ROWS) == chip, row, -1)

        rows = local_row(ids)
        lab_row = local_row(labs)
        mine = (rows >= 0).astype(F32)
        before = (jnp.arange(TOK)[:, None] < jnp.arange(TOK)[None, :]).astype(F32)
        rank = dot_plain(mine, before).astype(jnp.int32)
        slots = jnp.arange(CAP, dtype=jnp.int32)
        own_chip = ids[0] // (CHIP_ROWS)
        own_rel = jnp.bitwise_xor(own_chip, chip)
        is_rel = own_rel[None, :] == jnp.arange(NB)[:, None]
        own_rank_all = dot_plain(is_rel.astype(F32), before)
        own_rank = jnp.sum(jnp.where(is_rel, own_rank_all, 0.0), 0).astype(jnp.int32)
        counts = jnp.sum((both[:, 0] // (CHIP_ROWS))[:, None, :] == jnp.arange(NB)[None, :, None], axis=-1)
        rounds = (jnp.max(counts) + CAP - 1) // CAP

        def slot_rows(rnd):
            want = (rows[:, None, :] >= 0) & (rank[:, None, :] - rnd * CAP == slots[None, :, None])
            got = jnp.sum(jnp.where(want, rows[:, None, :] + 1, 0), axis=-1) - 1
            return got.reshape(SLOTS)

        def slot_tokens(rnd):
            want = is_rel[:, None, :] & (own_rank[None, None, :] - rnd * CAP == slots[None, :, None])
            return jnp.sum(jnp.where(want, jnp.arange(TOK)[None, None, :], 0), axis=-1).reshape(SLOTS)

        def lookup(rnd, x, cid):
            out = jnp.take(e_loc, jnp.maximum(slot_rows(rnd), 0), axis=0, mode='clip').reshape(NB, CAP, D)
            got = swap(out, cid).reshape(SLOTS, D)
            here = own_rank // CAP == rnd
            at = jnp.where(here, own_rel * CAP + own_rank % CAP, 0)
            return jnp.where(here[:, None], jnp.take(got, at, axis=0, mode='clip'), x)

        x_bf = lookup(0, jnp.zeros((TOK, D), BF), 3)
        x_bf = lax.while_loop(lambda c: c[0] < rounds, lambda c: (c[0] + 1, lookup(c[0], c[1], 4)), (jnp.int32(1), x_bf))[1]

        gm, gf = gain_mlp[None, :], gain_final[None, :]
        normed, gu, hidden_act, hid, hid_norm = mlp_forward(x_bf, gm, gf, w_gu, w_down)

        hn_all, lse = head_forward(hid_norm, e_loc)
        lab_pos = jnp.concatenate([lab_row[r, h * UNIT:(h + 1) * UNIT] for r, h in UNITS]).reshape(NB, 1, TB)
        d_hid, g_all, loss8 = head_backward(hn_all, e_loc, lse, lab_pos)

        slot = jnp.where(own_rank < CAP, own_rel * CAP + own_rank, -1)[None, :]
        d_down, d_gu, d_x, dxs = mlp_backward(d_hid, hid, x_bf, normed, gu, hidden_act, gm, gf, slot, w_gu, w_down)
        d_embed, d_gu, d_down, loss8, _ = last_sums(d_down, d_gu, dxs, slot_rows(0)[None, :], g_all, hn_all, loss8)
        loss = -jnp.sum(loss8) * (1.0 / TOTAL)

        def more(c):
            rnd, acc = c
            at = slot_rows(rnd)
            dx = swap(jnp.take(d_x, slot_tokens(rnd), axis=0, mode='clip').reshape(NB, CAP, D), 6).reshape(SLOTS, D)
            add = jnp.where((at >= 0)[:, None], dx.astype(F32) * EMB_SCALE, 0.0)
            part = jnp.zeros((VP, D), F32).at[jnp.maximum(at, 0)].add(add)
            pairs = [(d, d ^ 1) for d in range(NDEV)]
            return rnd + 1, acc + part[:SHARD] + lax.ppermute(part[HALF:HALF + SHARD], 'fsdp', pairs)

        d_embed = lax.while_loop(lambda c: c[0] < rounds, more, (jnp.int32(1), d_embed))[1]
        d_gu = d_gu.reshape(-1, NF, 2, FT)
        return loss, d_embed, d_gu[:, :, 0].reshape(-1, FF), d_gu[:, :, 1].reshape(-1, FF), d_down

    shard = P('fsdp', None)
    return jax.shard_map(local_step, mesh=mesh, in_specs=(shard,) * 6 + (P(), P()),
                         out_specs=(P(), shard, shard, shard, shard), check_vma=False)
```

```python
import functools
import math
import jax
import jax.numpy as jnp
from jax import lax
from jax.experimental import pallas as pl
from jax.experimental.pallas import tpu as pltpu
from jax.sharding import PartitionSpec as P

NORM_EPS = 1e-6
LOG2E = 1.4426950408889634
MESH = pl.DeviceIdType.MESH
ANY = pl.BlockSpec(memory_space=pl.ANY)
VMEM = pl.BlockSpec(memory_space=pltpu.VMEM)
BF = jnp.bfloat16
F32 = jnp.float32
DMA = pltpu.SemaphoreType.DMA

SHARD = 3144
HALF = 3200
VP = 2 * HALF
D = 768
FF = 3072
TOK = 512
UNIT = 256
NB = 8
TB = 512
GT = NB * TOK
VT = 1280
NT = VP // VT
NQ = NB * NT
CAP = 96
SLOTS = NB * CAP
TOTAL = 8192
NDEV = 2 * NB
CHIP_ROWS = 2 * SHARD
FF2 = 2 * FF
FT = 384
FT2 = 2 * FT
NF = FF // FT
EMB_SCALE = math.sqrt(D)

CUBE = range(NB)
AXES = range(3)
HALVES = range(2)


def unit_list(text):
    return [(int(r), 'ab'.index(h)) for r, h in zip(text[::2], text[1::2])]


UNITS = unit_list('0a0b2b1b4b1a4a2a3b6b5b3a6a5a7a7b')
BLOCKS = list(zip(UNITS[::2], UNITS[1::2]))
POS = {u: i for i, u in enumerate(UNITS)}
WAITS = {1: '2b1b4b', 2: '1a4a2a', 4: '3b6b5b', 5: '3a6a5a', 7: '7a7b'}
ROW, COL = D // 3, D // 2
CORNER = NB - 1
STAR = [(1 << a, a, 0, D) for a in AXES]
EDGE = [(CORNER - (1 << b), (b + 1 + j) % 3, j * COL, (j + 1) * COL) for b in (1, 0, 2) for j in HALVES]
TIP = [(CORNER, a, a * ROW, (a + 1) * ROW) for a in AXES]
SUMS = TIP + EDGE + STAR


def landing(path):
    s, a, lo, hi = path
    t = s - (1 << a)
    if s == CORNER:
        return 0, a, 0
    return (1, STAR_AT[t], lo) if t else (2, a, 0)


STAR_AT = {1 << a: a for a in AXES}


def dot_plain(a, b):
    return lax.dot_general(a, b, (((1,), (0,)), ((), ())), preferred_element_type=F32)


def dot_last(a, b):
    return lax.dot_general(a, b, (((1,), (1,)), ((), ())), preferred_element_type=F32)


def dot_first(a, b):
    return lax.dot_general(a, b, (((0,), (0,)), ((), ())), preferred_element_type=F32)


def one_hot(mask):
    return jnp.where(mask, 1.0, 0.0).astype(BF)


def peer_of(me, r):
    p = me
    for a in AXES:
        if r >> a & 1:
            step = 2 << a
            p = p + step - step * (me // step % 2 * 2)
    return p


def barrier_with(peers):
    sem = pltpu.get_barrier_semaphore()
    for p in peers:
        pl.semaphore_signal(sem, inc=1, device_id=(p,), device_id_type=MESH)
    pl.semaphore_wait(sem, len(peers))


def remote(src, dst, ssem, rsem, dev):
    return pltpu.make_async_remote_copy(src_ref=src, dst_ref=dst, send_sem=ssem, recv_sem=rsem,
                                        device_id=(dev,), device_id_type=MESH)


def params(cid, mib=60):
    return pltpu.CompilerParams(collective_id=cid, has_side_effects=True, vmem_limit_bytes=mib * 2 ** 20)


def pair_kernel(e_ref, out_ref, buf, zero, sems, ssem, rsem):
    me = lax.axis_index('fsdp')
    other = me + 1 - 2 * (me % 2)
    barrier_with([other])
    load = pltpu.make_async_copy(e_ref, buf, sems.at[0])
    load.start()
    zero[...] = jnp.zeros_like(zero)
    load.wait()
    send = remote(buf, out_ref.at[pl.ds(HALF, SHARD)], ssem, rsem, other)
    send.start()
    copies = [pltpu.make_async_copy(buf, out_ref.at[pl.ds(0, SHARD)], sems.at[1]),
              pltpu.make_async_copy(zero, out_ref.at[pl.ds(SHARD, HALF - SHARD)], sems.at[2]),
              pltpu.make_async_copy(zero, out_ref.at[pl.ds(HALF + SHARD, HALF - SHARD)], sems.at[3])]
    for c in copies:
        c.start()
    for c in copies:
        c.wait()
    send.wait()


def pair_gather(e_shard):
    return pl.pallas_call(
        pair_kernel, in_specs=[ANY], out_specs=ANY, out_shape=jax.ShapeDtypeStruct((VP, D), BF),
        scratch_shapes=[pltpu.VMEM((SHARD, D), BF), pltpu.VMEM((HALF - SHARD, D), BF), DMA((4,)),
                        DMA, DMA],
        compiler_params=params(0, 16), name='pair_gather')(e_shard)


def swap_kernel(in_ref, out_ref, recv, ssem, rsem):
    me = lax.axis_index('fsdp')
    peers = [peer_of(me, r) for r in range(1, NB)]
    barrier_with(peers)
    sends = [remote(in_ref.at[r], recv.at[r], ssem.at[r], rsem.at[r], peers[r - 1]) for r in range(1, NB)]
    for s in sends:
        s.start()
    out_ref[0] = in_ref[0]
    for r in range(1, NB):
        sends[r - 1].wait()
        out_ref[r] = recv[r]


def swap(rows, cid):
    return pl.pallas_call(
        swap_kernel, in_specs=[VMEM], out_specs=VMEM, out_shape=jax.ShapeDtypeStruct((NB, CAP, D), BF),
        scratch_shapes=[pltpu.VMEM((NB, CAP, D), BF), DMA((NB,)), DMA((NB,))],
        compiler_params=params(cid, 16), name='swap')(rows)


def mask_pads(s, j):
    for tile, at in ((2, SHARD - 2 * VT), (4, HALF + SHARD - 4 * VT)):
        rows = pl.ds(at, HALF - SHARD)
        s[rows, :] = jnp.where(j == tile, -jnp.inf, s[rows, :])


AG_PATHS = [(0, a, 0, D) for a in AXES] + [(1 << (a + 1) % 3, a, 0, D) for a in AXES] + [(CORNER - (1 << a), a, lo, hi) for _, a, lo, hi in TIP]
AG_LIST = [(s, h, a, lo, hi) for h in (1, 0) for (s, a, lo, hi) in AG_PATHS]


def fwd_kernel(hn_ref, e_ref, all_ref, lse_ref, e_v, hn_s, s0, s1, st, stat, csem, ssem, rsem, ssem2, rsem2):
    me = lax.axis_index('fsdp')
    nbr = [peer_of(me, 1 << a) for a in range(3)]
    peers = [peer_of(me, r) for r in range(1, NB)]
    barrier_with(peers)
    load_e = pltpu.make_async_copy(e_ref, e_v, csem.at[0])
    load_e.start()
    load_h = pltpu.make_async_copy(hn_ref, hn_s.at[pl.ds(0, TOK)], csem.at[1])
    load_h.start()
    load_h.wait()

    def piece(k):
        s, h, a, lo, hi = AG_LIST[k]
        src = hn_s.at[pl.ds(POS[(s, h)] * UNIT, UNIT), pl.ds(lo, hi - lo)]
        dst = hn_s.at[pl.ds(POS[(s ^ (1 << a), h)] * UNIT, UNIT), pl.ds(lo, hi - lo)]
        return remote(src, dst, ssem.at[k], rsem.at[k], nbr[a])

    def forward(unit):
        for k, (s, h, a, lo, hi) in enumerate(AG_LIST):
            if (s, h) == unit:
                piece(k).start()

    def arrive(units):
        for unit in units:
            for k, (s, h, a, lo, hi) in enumerate(AG_LIST):
                if (s ^ (1 << a), h) == unit:
                    piece(k).wait_recv()
            forward(unit)

    forward((0, 1))
    forward((0, 0))
    st[:, 0] = jnp.full((NB, 8, TB), -jnp.inf, F32)
    st[:, 1] = jnp.zeros((NB, 8, TB), F32)
    load_e.wait()

    def sdot(q):
        off = pl.multiple_of(lax.rem(q, NT) * VT, VT)
        tok = pl.multiple_of(lax.div(q, NT) * TB, TB)
        return dot_last(e_v[pl.ds(off, VT), :], hn_s[pl.ds(tok, TB), :])

    def proc(q, s):
        blk = lax.div(q, NT)
        s3 = s[...].reshape(VT // 8, 8, TB)
        m8 = st[blk, 0]
        nm = jnp.maximum(m8, s3.max(0))
        st[blk, 1] = st[blk, 1] * jnp.exp2((m8 - nm) * LOG2E) + jnp.exp2((s3 - nm[None]) * LOG2E).sum(0)
        st[blk, 0] = nm

    s0[...] = sdot(0)

    def body(i, carry):
        q = 2 * i
        for block, units in WAITS.items():
            @pl.when(i == (block * NT - 1) // 2)
            def _(units=units):
                arrive(unit_list(units))
        s1[...] = sdot(q + 1)
        mask_pads(s0, lax.rem(q, NT))
        proc(q, s0)
        s0[...] = sdot(jnp.minimum(q + 2, NQ - 1))
        mask_pads(s1, lax.rem(q + 1, NT))
        proc(q + 1, s1)
        return carry

    lax.fori_loop(0, NQ // 2, body, 0)
    out = pltpu.make_async_copy(hn_s, all_ref, csem.at[2])
    out.start()

    def unit_stat(unit):
        blk, at = POS[unit] // 2, (POS[unit] % 2) * UNIT
        m8, s8 = st[blk, 0, :, at:at + UNIT], st[blk, 1, :, at:at + UNIT]
        m = m8.max(0, keepdims=True)
        return m, (s8 * jnp.exp2((m8 - m) * LOG2E)).sum(0, keepdims=True)

    def stat_at(k, r):
        return stat.at[k, k ^ r, 0:1], stat.at[k, k ^ r, 1:2]

    for r in CUBE:
        for h in HALVES:
            for ref, val in zip(stat_at(0, r), unit_stat((r, h))):
                ref[:, h * UNIT:(h + 1) * UNIT] = val
    sends = [remote(stat.at[0], stat.at[r], ssem2.at[r], rsem2.at[r], peers[r - 1]) for r in range(1, NB)]
    for c in sends:
        c.start()
    for c in sends:
        c.wait()
    for r in CUBE:
        parts = [stat_at(k, r) for k in CUBE]
        top = functools.reduce(jnp.maximum, [m[...] for m, _ in parts])
        lse = top + jnp.log(sum(s[...] * jnp.exp2((m[...] - top) * LOG2E) for m, s in parts))
        for h in HALVES:
            blk, at = POS[(r, h)] // 2, (POS[(r, h)] % 2) * UNIT
            lse_ref[blk, :, at:at + UNIT] = lse[:, h * UNIT:(h + 1) * UNIT]
    for k in range(len(AG_LIST)):
        piece(k).wait_send()
    out.wait()


def head_forward(hn, e_loc):
    n = len(AG_LIST)
    return pl.pallas_call(
        fwd_kernel, in_specs=[ANY, ANY], out_specs=[ANY, VMEM],
        out_shape=[jax.ShapeDtypeStruct((GT, D), BF), jax.ShapeDtypeStruct((NB, 1, TB), F32)],
        scratch_shapes=[pltpu.VMEM((VP, D), BF), pltpu.VMEM((GT, D), BF), pltpu.VMEM((VT, TB), F32), pltpu.VMEM((VT, TB), F32),
                        pltpu.VMEM((NB, 2, 8, TB), F32), pltpu.VMEM((NB, NB, 2, TB), F32), DMA((3,)),
                        DMA((n,)), DMA((n,)),
                        DMA((NB,)), DMA((NB,))],
        compiler_params=params(1), name='head_fwd')(hn, e_loc)


RS_LIST = [(p, h) for p in SUMS for h in HALVES]


def bwd_kernel(hn_ref, e_ref, lse_ref, lab_ref, dh_ref, g_ref, l_ref,
               e_v, hn_s, s0, s1, g_s, dh, ra, rb, rc, csem, gsem, ssem, rsem):
    me = lax.axis_index('fsdp')
    nbr = [peer_of(me, 1 << a) for a in range(3)]
    barrier_with(nbr)
    load_e = pltpu.make_async_copy(e_ref, e_v, csem.at[0])
    load_e.start()
    load_h = pltpu.make_async_copy(hn_ref, hn_s, csem.at[1])
    load_h.start()
    dh[...] = jnp.zeros_like(dh)
    l_ref[...] = jnp.zeros_like(l_ref)
    bufs = (ra, rb, rc)

    def piece(k):
        (s, a, lo, hi), h = RS_LIST[k]
        src = dh.at[pl.ds(POS[(s, h)] * UNIT, UNIT), pl.ds(lo, hi - lo)]
        b, i, c = landing(RS_LIST[k][0])
        return remote(src, bufs[b].at[2 * i + h, :, pl.ds(c, hi - lo)], ssem.at[k], rsem.at[k], nbr[a])

    def finish(block):
        for r, half in BLOCKS[block]:
            rows = pl.ds(POS[(r, half)] * UNIT, UNIT)
            for k, (path, h) in enumerate(RS_LIST):
                s, a, lo, hi = path
                if (s ^ (1 << a), h) == (r, half):
                    piece(k).wait_recv()
                    b, i, c = landing(path)
                    dh[rows, lo:hi] += bufs[b][2 * i + h, :, c:c + hi - lo]
            for k, (path, h) in enumerate(RS_LIST):
                if (path[0], h) == (r, half):
                    piece(k).start()

    def place(q):
        return NB - 1 - lax.div(q, NT), pl.multiple_of(lax.rem(q, NT) * VT, VT)

    def sdot(q):
        blk, off = place(q)
        return dot_last(e_v[pl.ds(off, VT), :], hn_s[pl.ds(pl.multiple_of(blk * TB, TB), TB), :])

    iota = lax.broadcasted_iota(jnp.int32, (VT, TB), 0)

    def g_copy(i, k):
        blk, off = place(2 * i + k)
        at = 2 * lax.rem(i, 2) + k
        return pltpu.make_async_copy(g_s.at[at], g_ref.at[pl.ds(off, VT), pl.ds(pl.multiple_of(blk * TB, TB), TB)], gsem.at[at])

    def proc(i, k, s):
        blk, off = place(2 * i + k)
        mask_pads(s, lax.rem(2 * i + k, NT))
        w = s[...] - lse_ref[blk]
        hit = iota == (lab_ref[blk] - off)
        p = jnp.exp2(w * LOG2E - 13.0)
        gv = (p - jnp.where(hit, 2.0 ** -13, 0.0)).astype(BF)
        l_ref[...] += jnp.where(hit, w, 0.0).reshape(VT // 8, 8, TB).sum(0)
        g_s[2 * lax.rem(i, 2) + k] = gv
        rows = pl.ds(pl.multiple_of(blk * TB, TB), TB)
        dh[rows, :] += dot_first(gv, e_v[pl.ds(off, VT), :])

    load_e.wait()
    load_h.wait()
    s0[...] = sdot(0)

    def body(i, carry):
        @pl.when(i >= 2)
        def _():
            g_copy(i - 2, 0).wait()
            g_copy(i - 2, 1).wait()
        s1[...] = sdot(2 * i + 1)
        proc(i, 0, s0)
        s0[...] = sdot(jnp.minimum(2 * i + 2, NQ - 1))
        proc(i, 1, s1)
        g_copy(i, 0).start()
        g_copy(i, 1).start()
        for b in range(NB):
            @pl.when(i == (b * NT + NT - 1) // 2)
            def _(b=b):
                finish(NB - 1 - b)
        return carry

    lax.fori_loop(0, NQ // 2, body, 0)
    for i in (NQ // 2 - 2, NQ // 2 - 1):
        g_copy(i, 0).wait()
        g_copy(i, 1).wait()
    dh_ref[...] = dh[pl.ds(0, TOK), :]
    for k in range(len(RS_LIST)):
        piece(k).wait_send()


def head_backward(hn_all, e_loc, lse, lab):
    n = len(RS_LIST)
    return pl.pallas_call(
        bwd_kernel, in_specs=[ANY, ANY, VMEM, VMEM], out_specs=[VMEM, ANY, VMEM],
        out_shape=[jax.ShapeDtypeStruct((TOK, D), F32), jax.ShapeDtypeStruct((VP, GT), BF), jax.ShapeDtypeStruct((8, TB), F32)],
        scratch_shapes=[pltpu.VMEM((VP, D), BF), pltpu.VMEM((GT, D), BF), pltpu.VMEM((VT, TB), F32), pltpu.VMEM((VT, TB), F32),
                        pltpu.VMEM((4, VT, TB), BF), pltpu.VMEM((GT, D), F32),
                        pltpu.VMEM((6, UNIT, 256), F32), pltpu.VMEM((6, UNIT, D), F32), pltpu.VMEM((6, UNIT, D), F32),
                        DMA((2,)), DMA((4,)),
                        DMA((n,)), DMA((n,))],
        compiler_params=params(2), name='head_bwd')(hn_all, e_loc, lse, lab)


def rms_inv(values):
    return lax.rsqrt(jnp.mean(values * values, axis=-1, keepdims=True) + NORM_EPS)


def rms_backward(values, inv_rms, gain_vec, grad_out):
    scaled = grad_out * gain_vec
    return inv_rms * scaled - values * (inv_rms ** 3) * jnp.mean(scaled * values, axis=-1, keepdims=True)


ET = 320
HT = HALF // ET
NE = 2 * HT
GD = FF // NDEV
GU = D // NDEV
SUM_ORDER = [CORNER] + [p[0] for p in EDGE[::2] + STAR[::-1]] + [0]


def last_kernel(dhid_ref, h_ref, x_ref, a_ref, gu_ref, q_ref, wgu_ref, wd_ref, g_ref, hn_ref,
                gm_ref, gf_ref, slot_ref, rows_ref, perm_ref, l_ref,
                de_ref, ogate_ref, oup_ref, odd_ref, loss_ref, dx_ref, pe_ref,
                acc_d, acc_g, pair_d, pair_g, ra_d, ra_g, rb_d, rb_g, rc_d, rc_g, dxs, dxr, lbuf,
                pds, pdr, pgs, pgr, ssem, rsem, xs, xr, es, er, lsem, gsem, osem, csem, ls, lr, outsem):
    me = lax.axis_index('fsdp')
    core = me % 2
    other = me + 1 - 2 * core
    peers = [peer_of(me, r) for r in CUBE]
    far = [p + 1 - 2 * core for p in peers]
    everyone = peers[1:] + far
    barrier_with(everyone)

    lbuf[me] = sum(l_ref[:, k * 128:(k + 1) * 128] for k in range(TB // 128))
    loss_copies = [remote(lbuf.at[me], lbuf.at[me], ls.at[i], lr.at[i], p) for i, p in enumerate(everyone)]
    accs, pairs, sizes = (acc_d, acc_g), (pair_d, pair_g), (GD, GU)
    bufs = ((ra_d, ra_g), (rb_d, rb_g), (rc_d, rc_g))
    wide = (1, FF2 // D)

    def block(m, r):
        return pl.ds(pl.multiple_of(peers[r] // 2 * sizes[m], sizes[m]), sizes[m])

    def piece(m, k):
        s, a, lo, hi = SUMS[k]
        w = wide[m]
        b, i, c = landing(SUMS[k])
        return remote(accs[m].at[block(m, s), pl.ds(lo * w, (hi - lo) * w)], bufs[b][m].at[i, :, pl.ds(c * w, (hi - lo) * w)],
                      ssem.at[k, m], rsem.at[k, m], peers[1 << a])

    def add_pair(m, r):
        rows = block(m, r)
        accs[m][rows, :] += pairs[m][rows, :]

    def pass_on(m, r):
        w = wide[m]
        rows = block(m, r)
        for k, (s, a, lo, hi) in enumerate(SUMS):
            if s ^ (1 << a) == r:
                piece(m, k).wait_recv()
                b, i, c = landing(SUMS[k])
                accs[m][rows, lo * w:hi * w] += bufs[b][m][i, :, c * w:(c + hi - lo) * w]
        for k, (s, a, lo, hi) in enumerate(SUMS):
            if s == r:
                piece(m, k).start()

    def odd(t):
        return lax.rem(t, 2)

    def mlp(x_s, p_s, dm_s, dgu_s, dh_s, dn, q_t, wd_t, gu_t, wgu_t, tg):
        loads = [pltpu.make_async_copy(src, dst, csem.at[i]) for i, (src, dst) in
                 enumerate(((dhid_ref, dh_s), (h_ref, x_s), (a_ref, dgu_s), (x_ref, x_s)))]
        load_x = loads.pop()
        for c in loads:
            c.start()

        def cols(f, n):
            return pl.ds(pl.multiple_of(f * n, n), n)

        def q_load(f):
            return pltpu.make_async_copy(q_ref.at[:, cols(f, FT)], q_t.at[odd(f)], lsem.at[odd(f), 0])

        def w_loads(f):
            return [pltpu.make_async_copy(wd_ref.at[cols(f, FT)], wd_t.at[odd(f)], lsem.at[odd(f), 1]),
                    pltpu.make_async_copy(gu_ref.at[:, cols(f, FT2)], gu_t.at[odd(f)], lsem.at[odd(f), 2]),
                    pltpu.make_async_copy(wgu_ref.at[:, cols(f, FT2)], wgu_t.at[odd(f)], lsem.at[odd(f), 3])]

        def d_send(f):
            return remote(tg.at[odd(f), cols(1 - core, GD)], pair_d.at[cols(f, GD)],
                          pds.at[f], pdr.at[f], other)

        def g_send(f):
            return remote(tg.at[odd(f)], pair_g.at[:, cols(f, FT2)],
                          pgs.at[f], pgr.at[f], other)

        q_load(0).start()
        for c in w_loads(0):
            c.start()
        for c in loss_copies:
            c.start()
        for c in loads:
            c.wait()
        h = x_s[...].astype(F32)
        dh = rms_backward(h, rms_inv(h), gf_ref[...], dh_s[...])
        dh_s[...] = dh
        dm_s[...] = dh.astype(BF)
        dn[...] = jnp.zeros_like(dn)
        pick = lax.broadcasted_iota(jnp.int32, (D, D), 0) == perm_ref[...]
        p_s[...] = dot_plain(dgu_s[...], one_hot(pick)).astype(BF)
        load_x.start()

        def down(f, carry):
            @pl.when(f < NF - 1)
            def _():
                q_load(f + 1).start()

            @pl.when(f >= 2)
            def _():
                d_send(f - 2).wait_send()
            q_load(f).wait()
            tg[odd(f)] = dot_first(q_t[odd(f)], dm_s[...])
            acc_d[cols(f, GD), :] = tg[odd(f), cols(core, GD)]
            d_send(f).start()
            return carry

        def settle(send):
            for f in range(NF):
                send(f).wait_recv()
            for f in (NF - 2, NF - 1):
                send(f).wait_send()

        lax.fori_loop(0, NF, down, 0)
        settle(d_send)
        add_pair(0, CORNER)
        pass_on(0, CORNER)
        for r in SUM_ORDER[1:]:
            add_pair(0, r)

        def gate_up(f, carry):
            for when, rs in ((2, SUM_ORDER[1:4]), (NF - 1, SUM_ORDER[4:7])):
                @pl.when(f == when)
                def _(rs=rs):
                    for r in rs:
                        pass_on(0, r)

            @pl.when(f < NF - 1)
            def _():
                for c in w_loads(f + 1):
                    c.start()

            @pl.when(f >= 2)
            def _():
                g_send(f - 2).wait_send()
            for c in w_loads(f):
                c.wait()
            dq = dot_last(dm_s[...], wd_t[odd(f)])
            g, u = gu_t[odd(f), :, :FT].astype(F32), gu_t[odd(f), :, FT:].astype(F32)
            sig = jax.nn.sigmoid(g)
            dgu_s[:, :FT] = (dq * u * sig * (1.0 + g * (1.0 - sig))).astype(BF)
            dgu_s[:, FT:] = (dq * g * sig).astype(BF)
            tg[odd(f)] = dot_first(p_s[:, FT:], dgu_s[...])
            g_send(f).start()
            acc_g[:, cols(f, FT2)] = dot_first(p_s[:, :FT], dgu_s[...])
            dn[...] += dot_last(dgu_s[...], wgu_t[odd(f)])
            return carry

        lax.fori_loop(0, NF, gate_up, 0)
        load_x.wait()
        x = x_s[...].astype(F32) * EMB_SCALE
        dx = (dh_s[...] + rms_backward(x, rms_inv(x), gm_ref[...], dn[...])).astype(BF)
        dx_ref[...] = dx
        pick = lax.broadcasted_iota(jnp.int32, (SLOTS, TOK), 0) == slot_ref[...]
        dxs[...] = dot_plain(one_hot(pick), dx).astype(BF)
        settle(g_send)

    pl.run_scoped(mlp, *[pltpu.VMEM((TOK, D), BF)] * 4, *[pltpu.VMEM((TOK, D), F32)] * 2,
                  *[pltpu.VMEM((2, *shape), BF) for shape in ((TOK, FT), (FT, D), (TOK, FT2), (D, FT2))], pltpu.VMEM((2, FT, D), F32))

    dx_copies = [remote(dxs.at[pl.ds(r * CAP, CAP)], dxr.at[pl.ds(r * CAP, CAP)], xs.at[r], xr.at[r], peers[r])
                 for r in range(1, NB)]
    add_pair(1, CORNER)
    pass_on(1, CORNER)
    for c in dx_copies:
        c.start()
    dxr[pl.ds(0, CAP)] = dxs[pl.ds(0, CAP)]
    for r in SUM_ORDER[1:]:
        add_pair(1, r)

    def embed(hn_s, g_s, ob, pb):
        load_h = pltpu.make_async_copy(hn_ref, hn_s, csem.at[0])
        load_h.start()

        def g_load(t):
            off = pl.multiple_of(lax.rem(t + HT, NE) * ET, ET)
            return pltpu.make_async_copy(g_ref.at[pl.ds(off, ET)], g_s.at[odd(t)], gsem.at[odd(t)])

        def e_send(t):
            return remote(ob.at[odd(t)], pe_ref.at[pl.ds(pl.multiple_of(t * ET, ET), ET)], es.at[t], er.at[t], other)

        def e_out(t, n=ET):
            at = pl.multiple_of((t - HT) * ET, ET)
            return pltpu.make_async_copy(ob.at[odd(t), pl.ds(0, n)], de_ref.at[pl.ds(at, n)], osem.at[odd(t)])

        def e_load(t):
            return pltpu.make_async_copy(pe_ref.at[pl.ds(pl.multiple_of((t - HT) * ET, ET), ET)], pb, csem.at[1])

        g_load(0).start()
        load_h.wait()
        for c in dx_copies:
            c.wait_recv()
        iota = lax.broadcasted_iota(jnp.int32, (ET, SLOTS), 0)
        last = SHARD - (HT - 1) * ET

        def body(t, carry):
            for when, rs in ((HT - 2, SUM_ORDER[1:4]), (NE - 1, SUM_ORDER[4:7])):
                @pl.when(t == when)
                def _(rs=rs):
                    for r in rs:
                        pass_on(1, r)

            @pl.when((t >= 2) & (t < HT + 2))
            def _():
                e_send(t - 2).wait_send()

            @pl.when(t >= HT + 2)
            def _():
                e_out(t - 2).wait()

            @pl.when(t >= HT)
            def _():
                e_send(t - HT).wait_recv()
                e_load(t).start()

            @pl.when(t < NE - 1)
            def _():
                g_load(t + 1).start()
            g_load(t).wait()
            base = lax.rem(t + HT, NE) * ET
            pick = one_hot(iota == rows_ref[...] - base)
            ob[odd(t)] = dot_plain(g_s[odd(t)], hn_s[...]) + dot_plain(pick, dxr[...]) * EMB_SCALE

            @pl.when(t < HT)
            def _():
                e_send(t).start()

            @pl.when(t >= HT)
            def _():
                e_load(t).wait()
                ob[odd(t)] += pb[...]

            @pl.when((t >= HT) & (t < NE - 1))
            def _():
                e_out(t).start()

            @pl.when(t == NE - 1)
            def _():
                e_out(t, last).start()
            return carry

        lax.fori_loop(0, NE, body, 0)
        e_out(NE - 2).wait()
        e_out(NE - 1, last).wait()

    pl.run_scoped(embed, pltpu.VMEM((GT, D), BF), pltpu.VMEM((2, ET, GT), BF), pltpu.VMEM((2, ET, D), F32), pltpu.VMEM((ET, D), F32))
    for c in loss_copies:
        c.wait()
    tot = lbuf[0]
    for i in range(1, NDEV):
        tot = tot + lbuf[i]
    loss_ref[...] = tot
    for m in HALVES:
        pass_on(m, 0)
    outs = [pltpu.make_async_copy(acc_d.at[block(0, 0)], odd_ref, gsem.at[0])]
    for f in range(NF):
        for i, out in enumerate((ogate_ref, oup_ref)):
            part = acc_g.at[block(1, 0), pl.ds((2 * f + i) * FT, FT)]
            outs.append(pltpu.make_async_copy(part, out.at[:, pl.ds(f * FT, FT)], outsem.at[f, i]))
    for c in outs:
        c.start()
    for c in outs:
        c.wait()
    for c in dx_copies:
        c.wait_send()
    for m in HALVES:
        for k in range(len(SUMS)):
            piece(m, k).wait_send()


def last_sums(*args):
    n = len(SUMS)
    scr = [pltpu.VMEM(shape, F32) for shape in ((NB * GD, D), (NB * GU, FF2)) * 2 + (
        (3, GD, ROW), (3, GU, ROW * FF2 // D)) + ((3, GD, D), (3, GU, FF2)) * 2]
    scr += [pltpu.VMEM((SLOTS, D), BF), pltpu.VMEM((SLOTS, D), BF), pltpu.VMEM((NDEV, 8, 128), F32)]
    scr += [DMA((k,)) for k in (NF,) * 4] + [DMA((n, 2)), DMA((n, 2))] + [DMA((k,)) for k in (NB, NB, HT, HT)]
    scr += [DMA((2, 4)), DMA((2,)), DMA((2,)), DMA((4,)), DMA((NDEV - 1,)), DMA((NDEV - 1,)), DMA((NF, 2))]
    shapes = ((SHARD, D), (GU, FF), (GU, FF), (GD, D), (8, 128))
    return pl.pallas_call(
        last_kernel, in_specs=[ANY] * 10 + [VMEM] * 6, out_specs=[ANY] * 4 + [VMEM] * 2 + [ANY],
        out_shape=[jax.ShapeDtypeStruct(shape, F32) for shape in shapes] + [
            jax.ShapeDtypeStruct((TOK, D), BF), jax.ShapeDtypeStruct((HALF, D), F32)],
        scratch_shapes=scr, compiler_params=params(7, 63), name='last_sums')(*args)


def mlp_fwd_kernel(x_ref, gm_ref, gf_ref, wgu_ref, wd_ref, a_ref, gu_ref, q_ref, h_ref, hn_ref, acc):
    f = pl.program_id(0)

    @pl.when(f == 0)
    def _():
        x = x_ref[...].astype(F32) * EMB_SCALE
        a_ref[...] = (x * rms_inv(x) * gm_ref[...]).astype(BF)
        acc[...] = jnp.zeros_like(acc)
    gu = dot_plain(a_ref[...], wgu_ref[...]).astype(BF)
    gu_ref[...] = gu
    g, u = gu[:, :FT].astype(F32), gu[:, FT:].astype(F32)
    q = (g * jax.nn.sigmoid(g) * u).astype(BF)
    q_ref[...] = q
    acc[...] += dot_plain(q, wd_ref[...])

    @pl.when(f == NF - 1)
    def _():
        x = x_ref[...].astype(F32) * EMB_SCALE
        h = (x + acc[...].astype(BF).astype(F32)).astype(BF)
        h_ref[...] = h
        h = h.astype(F32)
        hn_ref[...] = (h * rms_inv(h) * gf_ref[...]).astype(BF)


def whole(shape):
    return pl.BlockSpec(shape, lambda f: (0, 0))


def mlp_forward(x, gain_mlp, gain_final, w_gu, w_down):
    tok = jax.ShapeDtypeStruct((TOK, D), BF)
    return pl.pallas_call(
        mlp_fwd_kernel, grid=(NF,),
        in_specs=[whole((TOK, D)), whole((1, D)), whole((1, D)), pl.BlockSpec((D, FT2), lambda f: (0, f)),
                  pl.BlockSpec((FT, D), lambda f: (f, 0))],
        out_specs=[whole((TOK, D)), pl.BlockSpec((TOK, FT2), lambda f: (0, f)), pl.BlockSpec((TOK, FT), lambda f: (0, f)),
                   whole((TOK, D)), whole((TOK, D))],
        out_shape=[tok, jax.ShapeDtypeStruct((TOK, FF2), BF), jax.ShapeDtypeStruct((TOK, FF), BF), tok, tok],
        scratch_shapes=[pltpu.VMEM((TOK, D), F32)],
        compiler_params=pltpu.CompilerParams(vmem_limit_bytes=40 * 2 ** 20), name='mlp_fwd')(x, gain_mlp, gain_final, w_gu, w_down)


def join_parts(gate, up):
    return jnp.concatenate([w[:, f * FT:(f + 1) * FT] for f in range(NF) for w in (gate, up)], 1)


def solution(mesh):
    def local_step(ids_blk, lab_blk, emb_shard, gate_shard, up_shard, down_shard, gain_mlp, gain_final):
        me = lax.axis_index('fsdp')
        core, chip = me % 2, me // 2
        both = lax.all_gather(jnp.concatenate([ids_blk, lab_blk]), 'fsdp')
        w_gu = lax.all_gather(join_parts(gate_shard, up_shard), 'fsdp', tiled=True)
        w_down = lax.all_gather(down_shard, 'fsdp', tiled=True)
        e_loc = pair_gather(emb_shard)

        rel = jnp.stack([peer_of(me, r) for r in range(NB)])
        grp = jnp.take(both, rel, axis=0)
        ids, labs = grp[:, 0], grp[:, 1]

        def mid(v):
            return jnp.expand_dims(v, 1)

        def local_row(v):
            within = v % (CHIP_ROWS)
            row = jnp.where(within // SHARD == core, 0, HALF) + within % SHARD
            return jnp.where(v // (CHIP_ROWS) == chip, row, -1)

        rows = local_row(ids)
        lab_row = local_row(labs)
        mine = (rows >= 0).astype(F32)
        before = jnp.triu(jnp.ones((TOK, TOK), F32), 1)
        rank = dot_plain(mine, before).astype(jnp.int32)
        slots = jnp.arange(CAP).reshape(CAP, 1)
        own_chip = ids[0] // (CHIP_ROWS)
        own_rel = jnp.bitwise_xor(own_chip, chip)
        is_rel = own_rel == jnp.arange(NB).reshape(NB, 1)
        own_rank_all = dot_plain(is_rel.astype(F32), before)
        own_rank = jnp.sum(jnp.where(is_rel, own_rank_all, 0.0), 0).astype(jnp.int32)
        counts = jnp.sum(both[:, :1] // CHIP_ROWS == jnp.arange(NB).reshape(NB, 1), axis=-1)
        rounds = (jnp.max(counts) + CAP - 1) // CAP

        def slot_rows(rnd):
            row, at = mid(rows), mid(rank)
            got = jnp.sum(jnp.where((row >= 0) & (at - rnd * CAP == slots), row + 1, 0), axis=-1) - 1
            return got.reshape(SLOTS)

        def slot_tokens(rnd):
            want = mid(is_rel) & (own_rank - rnd * CAP == slots)
            return jnp.sum(jnp.where(want, jnp.arange(TOK), 0), axis=-1).reshape(SLOTS)

        def lookup(rnd, x, cid):
            out = jnp.take(e_loc, jnp.maximum(slot_rows(rnd), 0), axis=0, mode='clip').reshape(NB, CAP, D)
            got = swap(out, cid).reshape(SLOTS, D)
            here = own_rank // CAP == rnd
            at = jnp.where(here, own_rel * CAP + own_rank % CAP, 0)
            return jnp.where(here[:, None], jnp.take(got, at, axis=0, mode='clip'), x)

        x_bf = lookup(0, jnp.zeros((TOK, D), BF), 3)
        x_bf = lax.while_loop(lambda c: c[0] < rounds, lambda c: (c[0] + 1, lookup(c[0], c[1], 4)), (jnp.int32(1), x_bf))[1]

        gm, gf = gain_mlp[None, :], gain_final[None, :]
        normed, gu, hidden_act, hid, hid_norm = mlp_forward(x_bf, gm, gf, w_gu, w_down)

        hn_all, lse = head_forward(hid_norm, e_loc)
        lab_pos = jnp.concatenate([lab_row[r, h * UNIT:(h + 1) * UNIT] for r, h in UNITS]).reshape(NB, 1, TB)
        d_hid, g_all, loss8 = head_backward(hn_all, e_loc, lse, lab_pos)

        slot = jnp.where(own_rank < CAP, own_rel * CAP + own_rank, -1)[None, :]
        cols = jnp.arange(D).reshape(NB, 2, GU)
        perm = jnp.concatenate([jnp.take(cols, k, axis=1).reshape(1, -1) for k in (core, 1 - core)], 1)
        d_embed, d_gate, d_up, d_down, loss8, d_x, _ = last_sums(
            d_hid, hid, x_bf, normed, gu, hidden_act, w_gu, w_down, g_all, hn_all,
            gm, gf, slot, slot_rows(0)[None, :], perm, loss8)
        loss = -jnp.sum(loss8) * (1.0 / TOTAL)

        def more(c):
            rnd, acc = c
            at = slot_rows(rnd)
            dx = swap(jnp.take(d_x, slot_tokens(rnd), axis=0, mode='clip').reshape(NB, CAP, D), 6).reshape(SLOTS, D)
            add = jnp.where((at >= 0)[:, None], dx.astype(F32) * EMB_SCALE, 0.0)
            part = jnp.zeros((VP, D), F32).at[jnp.maximum(at, 0)].add(add)
            pairs = [(d, d ^ 1) for d in range(NDEV)]
            return rnd + 1, acc + part[:SHARD] + lax.ppermute(part[HALF:HALF + SHARD], 'fsdp', pairs)

        d_embed = lax.while_loop(lambda c: c[0] < rounds, more, (jnp.int32(1), d_embed))[1]
        return loss, d_embed, d_gate, d_up, d_down

    shard = P('fsdp', None)
    return jax.shard_map(local_step, mesh=mesh, in_specs=(shard,) * 6 + (P(), P()),
                         out_specs=(P(), shard, shard, shard, shard), check_vma=False)
```
